32 devices in a mesh: mem: 8 (over z, y), dom: 4 (over x, core).
Axes of the slice: x: 2, y: 2, z: 4, core: 2. Of those that a mesh axis runs over, the one named last changes fastest.
Arguments:
- particle_states: float32 [64, 3, 256, 1024], P('mem', None, 'dom'), may hold values from -6 to 6
- coriolis: float32 [256], replicated, may hold values from -0.6 to 0.6
- observed_cells: int32 [4, 64, 512], P('dom', 'mem'), may hold values from 0 to 1023
- observed_values: float32 [4, 64, 512], P('dom', 'mem'), may hold values from -6 to 15
- resample_draws: int32 [4, 64, 8, 192], P('dom', 'mem'), may hold values from 0 to 63
Outputs:
- analysed: float32 [64, 3, 256, 1024], P('mem', None, 'dom')
The draws below stay inside these ranges and needn't reach their ends.
All inputs are finite; a program needn't handle non-finite values.
Results may differ from the reference program's by a relative error of at most 0.0003.
Values sent between devices are 32-bit elements; how exact they have to be, the bound alone decides.
No kernel may reach another device: no remote copies, remote signals or barrier semaphores. Data moves between devices by JAX's collectives and lax.ppermute only.
A program may use at most 128 MiB of HBM per device.

```python
import jax
import jax.numpy as jnp
from jax import lax

ROWS_DEV = 64
NLON = 1024
NOBS = 512
LBLK = 128
LOC = 64
STEPS = 2
ENS = 64
NLAT = 256
NBLK = 8
N_DOM = 4


def draw_observed_values(key, part):
    normal_part = jnp.clip(jax.random.normal(jax.random.fold_in(key, 11), (N_DOM, ROWS_DEV, NOBS), jnp.float32), -6.0, 6.0)
    return normal_part


def place_ends(array, stream_key, low, high):
    longest = array.shape.index(max(array.shape))
    spots = []
    for shift in (0, 1):
        where = [jax.random.randint(jax.random.fold_in(stream_key, axis), (), 0, length) for axis, length in enumerate(array.shape)]
        where[longest] = (where[longest] + shift) % array.shape[longest]
        spots.append(tuple(where))
    return array.at[spots[0]].set(low).at[spots[1]].set(high)


def block_levels(stream_key, extent, cuts, least, high):
    level, own = 1.0, jax.random.fold_in(stream_key, 6)
    for dim, blocks in cuts:
        steps = jnp.exp(jax.random.uniform(jax.random.fold_in(own, dim), (blocks,), jnp.float32, least / len(cuts), high / len(cuts)))
        level = level * jnp.repeat(steps, extent[dim] // blocks).reshape([-1 if axis == dim else 1 for axis in range(len(extent))])
    return level


def bell_draw(key, extent, spread, reach, cuts=(), held_as=jnp.bfloat16):
    array = jax.random.normal(key, extent, jnp.float32) * spread
    if len(cuts) > 0:
        array = block_levels(key, extent, cuts, -0.22, 0.18) * array
    return jnp.clip(array, min=-reach, max=reach).astype(held_as)


def setup_inputs(seed: int = 0) -> dict:
    key_of = jax.random.split(jax.random.key(seed), 6)
    particle_states = bell_draw(key_of[0], (ENS, 3, NLAT, NLON), 1.0, 6.0, ((0, 8), (2, 4)), jnp.float32)
    coriolis = jnp.clip(jax.random.uniform(key_of[1], (NLAT,), jnp.float32, -0.6, 0.6), -0.6, 0.6)
    observed_cells = place_ends(jax.random.randint(key_of[2], (N_DOM, ROWS_DEV, NOBS), 0, NLON), jax.random.fold_in(key_of[2], 1), 0, NLON - 1).astype(jnp.int32)
    observed_values = draw_observed_values(jax.random.fold_in(key_of[5], 71), 0)
    resample_draws = place_ends(jax.random.randint(key_of[4], (N_DOM, ROWS_DEV, NBLK, 3 * ENS), 0, ENS), jax.random.fold_in(key_of[4], 1), 0, ENS - 1).astype(jnp.int32)
    return {"particle_states": particle_states, "coriolis": coriolis, "observed_cells": observed_cells, "observed_values": observed_values, "resample_draws": resample_draws}


FLOW_FACTOR = 1.0
PRESSURE_FACTOR = 1.0
OBSERVATION_VARIANCE = 16.0
RELAXATION = 0.5
MERGE_FIRST = 0.75
BLEND_COEF_TWO = (13.0 ** 0.5 + 1.0) / 8.0
MERGE_THIRD = -(13.0 ** 0.5 - 1.0) / 8.0


def along_east(quantity):
    return 0.5 * (jnp.roll(quantity, -1, axis=-1) - jnp.roll(quantity, 1, axis=-1))


def meridional_offset(quantity):
    border = jnp.zeros_like(quantity[..., :1, :])
    upper = jnp.concatenate([quantity[..., 1:, :], border], axis=-2)
    lower = jnp.concatenate([border, quantity[..., :-1, :]], axis=-2)
    return 0.5 * (upper - lower)


def advance(height, east_wind, north_wind, coriolis_col, inside):
    height_new = (height - FLOW_FACTOR * (along_east(east_wind) + meridional_offset(north_wind))) * inside
    east_new = (east_wind - PRESSURE_FACTOR * along_east(height_new) + coriolis_col * north_wind) * inside
    north_updated = (north_wind - PRESSURE_FACTOR * meridional_offset(height_new) - coriolis_col * east_wind) * inside
    return height_new, east_new, north_updated


def tapering(cells, grid_width, block_cells, length):
    longitude = cells.astype(jnp.float32)
    tile_total = grid_width // block_cells
    centre = jnp.arange(tile_total).astype(jnp.float32) * block_cells + 0.5 * (block_cells - 1)
    distance = jnp.abs(longitude[..., :, None] - centre)
    distance = jnp.minimum(distance, grid_width - distance)
    return jnp.exp(-0.5 * (distance / length) ** 2)


def member_weights(heights, cells, values, block_cells, length):
    grid_width = heights.shape[-1]
    chosen_cells = (cells[:, None, :] == lax.broadcasted_iota(jnp.int32, (1, grid_width, 1), 1)).astype(jnp.float32)
    observed = jnp.einsum("erl,rlo->reo", heights, chosen_cells, precision=lax.Precision.HIGHEST)
    misfit = (values[:, None, :] - observed) ** 2
    taper_weights = tapering(cells, grid_width, block_cells, length)
    likelihood = (-0.5 / OBSERVATION_VARIANCE) * jnp.einsum("reo,rob->rbe", misfit, taper_weights, precision=lax.Precision.HIGHEST)
    largest = jnp.max(likelihood, axis=-1, keepdims=True)
    scaled = jnp.exp(likelihood - largest)
    return scaled / jnp.sum(scaled, axis=-1, keepdims=True)


def merge_members(members, weights, draws, block_cells):
    member_count, fields, count_of_rows, grid_width = members.shape
    tile_total = grid_width // block_cells
    split = draws.reshape(draws.shape[:-1] + (3, member_count))
    column = lax.broadcasted_iota(jnp.int32, (1, 1, 1, member_count), 3)
    picks = MERGE_FIRST * (split[:, :, 0, :, None] == column).astype(jnp.float32)
    picks = picks + BLEND_COEF_TWO * (split[:, :, 1, :, None] == column).astype(jnp.float32)
    picks = picks + MERGE_THIRD * (split[:, :, 2, :, None] == column).astype(jnp.float32)
    mixing_weights = (1.0 - RELAXATION) * weights[:, :, None, :] + RELAXATION * picks
    blocks = members.reshape(member_count, fields, count_of_rows, tile_total, block_cells)
    updated = jnp.einsum("rbek,kfrbc->efrbc", mixing_weights, blocks, precision=lax.Precision.HIGHEST)
    return updated.reshape(member_count, fields, count_of_rows, grid_width)


def reference(particle_states, coriolis, observed_cells, observed_values, resample_draws):
    grid_rows = particle_states.shape[2]
    coriolis_col = coriolis[:, None]
    inside = jnp.ones_like(coriolis_col)

    def prior_states(particle_number):
        height, east_wind, north_wind = particle_number[0], particle_number[1], particle_number[2]
        for iteration_number in range(STEPS):
            height, east_wind, north_wind = advance(height, east_wind, north_wind, coriolis_col, inside)
        return jnp.stack([height, east_wind, north_wind])

    prior_estimates = lax.map(prior_states, particle_states)
    cells_all = observed_cells.reshape(grid_rows, NOBS)
    values_all = observed_values.reshape(grid_rows, NOBS)
    draws_all = resample_draws.reshape(grid_rows, NBLK, 3 * ENS)

    def one_row(row_index, analysed):
        row_index = jnp.asarray(row_index).astype(jnp.int32)
        members = lax.dynamic_slice_in_dim(prior_estimates, row_index, 1, axis=2)
        cells = lax.dynamic_slice_in_dim(cells_all, row_index, 1, axis=0)
        values = lax.dynamic_slice_in_dim(values_all, row_index, 1, axis=0)
        draws = lax.dynamic_slice_in_dim(draws_all, row_index, 1, axis=0)
        weights = member_weights(members[:, 0], cells, values, LBLK, LOC)
        updated = merge_members(members, weights, draws, LBLK)
        return lax.dynamic_update_slice_in_dim(analysed, updated, row_index, axis=2)

    return lax.fori_loop(0, grid_rows, one_row, jnp.zeros_like(prior_estimates))
```

```python
import jax
import jax.numpy as jnp
from jax import lax
from jax.sharding import PartitionSpec as P

LBLK = 128
LOC = 64
STEPS = 2


FLOW_FACTOR = 1.0
PRESSURE_FACTOR = 1.0
OBSERVATION_VARIANCE = 16.0
RELAXATION = 0.5
MERGE_FIRST = 0.75
BLEND_COEF_TWO = (13.0**0.5 + 1.0) / 8.0
MERGE_THIRD = -(13.0**0.5 - 1.0) / 8.0


def with_halo(array, sides, width):
    for axis, dim in sides:
        count, length = (lax.axis_size(axis), array.shape[dim])
        up = [(i, (i + 1) % count) for i in range(count - 1)]
        down = [(j, i) for i, j in up]
        last = lax.slice_in_dim(array, length - width, length, axis=dim)
        leading = lax.slice_in_dim(array, 0, width, axis=dim)
        before = lax.ppermute(last, axis, up)
        after = lax.ppermute(leading, axis, down)
        array = jnp.concatenate([before, array, after], axis=dim)
    return array


def along_east(quantity):
    return 0.5 * (jnp.roll(quantity, -1, axis=-1) - jnp.roll(quantity, 1, axis=-1))


def meridional_offset(quantity):
    border = jnp.zeros_like(quantity[..., :1, :])
    upper = jnp.concatenate([quantity[..., 1:, :], border], axis=-2)
    lower = jnp.concatenate([border, quantity[..., :-1, :]], axis=-2)
    return 0.5 * (upper - lower)


def advance(height, east_wind, north_wind, coriolis_col, inside):
    height_new = (
        height - FLOW_FACTOR * (along_east(east_wind) + meridional_offset(north_wind))
    ) * inside
    east_new = (
        east_wind - PRESSURE_FACTOR * along_east(height_new) + coriolis_col * north_wind
    ) * inside
    north_updated = (
        north_wind - PRESSURE_FACTOR * meridional_offset(height_new) - coriolis_col * east_wind
    ) * inside
    return (height_new, east_new, north_updated)


def tapering(cells, grid_width, block_cells, length):
    longitude = cells.astype(jnp.float32)
    tile_total = grid_width // block_cells
    centre = jnp.arange(tile_total).astype(jnp.float32) * block_cells + 0.5 * (block_cells - 1)
    distance = jnp.abs(longitude[..., :, None] - centre)
    distance = jnp.minimum(distance, grid_width - distance)
    return jnp.exp(-0.5 * (distance / length) ** 2)


def member_weights(heights, cells, values, block_cells, length):
    grid_width = heights.shape[-1]
    chosen_cells = (
        cells[:, None, :] == lax.broadcasted_iota(jnp.int32, (1, grid_width, 1), 1)
    ).astype(jnp.float32)
    observed = jnp.einsum("erl,rlo->reo", heights, chosen_cells, precision=lax.Precision.HIGHEST)
    misfit = (values[:, None, :] - observed) ** 2
    taper_weights = tapering(cells, grid_width, block_cells, length)
    likelihood = (
        -0.5
        / OBSERVATION_VARIANCE
        * jnp.einsum("reo,rob->rbe", misfit, taper_weights, precision=lax.Precision.HIGHEST)
    )
    largest = jnp.max(likelihood, axis=-1, keepdims=True)
    scaled = jnp.exp(likelihood - largest)
    return scaled / jnp.sum(scaled, axis=-1, keepdims=True)


def mixing_matrix(weights, draws):
    member_count = weights.shape[-1]
    split = draws.reshape(draws.shape[:-1] + (3, member_count))
    column = lax.broadcasted_iota(jnp.int32, (1, 1, 1, member_count), 3)
    picks = MERGE_FIRST * (split[:, :, 0, :, None] == column).astype(jnp.float32)
    picks = picks + BLEND_COEF_TWO * (split[:, :, 1, :, None] == column).astype(jnp.float32)
    picks = picks + MERGE_THIRD * (split[:, :, 2, :, None] == column).astype(jnp.float32)
    return (1.0 - RELAXATION) * weights[:, :, None, :] + RELAXATION * picks


def merge_field(members, mixing, block_cells):
    member_count, count_of_rows, grid_width = members.shape
    blocks = members.reshape(member_count, count_of_rows, grid_width // block_cells, block_cells)
    updated = jnp.einsum("rbek,krbc->erbc", mixing, blocks, precision=lax.Precision.HIGHEST)
    return updated.reshape(member_count, count_of_rows, grid_width)


def band_tables(coriolis, band_index, count_of_rows, margin):
    grid_rows = coriolis.shape[0]
    padded = jnp.pad(coriolis, (margin, margin))
    band_rows = lax.dynamic_slice_in_dim(
        padded, band_index * count_of_rows, count_of_rows + 2 * margin
    )
    position = (
        band_index * count_of_rows
        - margin
        + jnp.arange(count_of_rows + 2 * margin, dtype=jnp.int32)
    )
    inside = ((position >= 0) & (position < grid_rows)).astype(jnp.float32)
    return (band_rows[:, None], inside[:, None])


def body(particle_states, coriolis, observed_cells, observed_values, resample_draws):
    count_of_rows = particle_states.shape[2]
    band_index = lax.axis_index("dom")
    margin = 2 * STEPS
    coriolis_col, inside = band_tables(coriolis, band_index, count_of_rows, margin)
    padded = with_halo(particle_states, (("dom", 2),), 2 * STEPS)
    height, east_wind, north_wind = (padded[:, 0], padded[:, 1], padded[:, 2])
    for iteration_number in range(STEPS):
        height, east_wind, north_wind = advance(height, east_wind, north_wind, coriolis_col, inside)
    cells = observed_cells[0]
    values = observed_values[0]
    draws = resample_draws[0]
    gathered = [
        lax.all_to_all(
            field[:, margin : margin + count_of_rows], "mem", split_axis=1, concat_axis=0, tiled=True
        )
        for field in (height, east_wind, north_wind)
    ]
    weights = member_weights(gathered[0], cells, values, LBLK, LOC)
    mixing = mixing_matrix(weights, draws)
    returned = [
        lax.all_to_all(
            merge_field(field, mixing, LBLK), "mem", split_axis=0, concat_axis=1, tiled=True
        )
        for field in gathered
    ]
    return jnp.stack(returned, axis=1)


def solution(mesh):
    return jax.shard_map(
        body,
        mesh=mesh,
        in_specs=(
            P("mem", None, "dom", None),
            P(),
            P("dom", "mem", None),
            P("dom", "mem", None),
            P("dom", "mem", None, None),
        ),
        out_specs=P("mem", None, "dom", None),
        check_vma=False,
    )
```

```python
import functools

import jax
import jax.numpy as jnp
from jax import lax
from jax.experimental import pallas as pl
from jax.experimental.pallas import tpu as pltpu
from jax.sharding import PartitionSpec as P

LBLK = 128
LOC = 64
STEPS = 2
SUBLANES = 8
LANES = 128


FLOW_FACTOR = 1.0
PRESSURE_FACTOR = 1.0
OBSERVATION_VARIANCE = 16.0
RELAXATION = 0.5
MERGE_FIRST = 0.75
BLEND_COEF_TWO = (13.0**0.5 + 1.0) / 8.0
MERGE_THIRD = -(13.0**0.5 - 1.0) / 8.0


def edge_rows(array, axis, dim, width):
    count, length = (lax.axis_size(axis), array.shape[dim])
    up = [(i, i + 1) for i in range(count - 1)]
    down = [(j, i) for i, j in up]
    before = lax.ppermute(lax.slice_in_dim(array, length - width, length, axis=dim), axis, up)
    after = lax.ppermute(lax.slice_in_dim(array, 0, width, axis=dim), axis, down)
    return before, after


def forecast_kernel(margin, inside_ref, coriolis_ref, states_ref, before_ref, after_ref,
                    height_ref, winds_ref, here, there):
    rows, width = states_ref.shape[2:]
    last = rows // SUBLANES + 2
    first_row = 2 * SUBLANES

    def tile(t, shift=0):
        return slice(t * SUBLANES + shift, (t + 1) * SUBLANES + shift)

    def east(quantity):
        return pltpu.roll(quantity, width - 1, 1) - pltpu.roll(quantity, 1, 1)

    def north(ref, field, t):
        return ref[field, tile(t, 1), :] - ref[field, tile(t, -1), :]

    def masked(quantity, t):
        if t == 1:
            return quantity * inside_ref[0]
        if t == last:
            return quantity * inside_ref[1]
        return quantity

    here[:, first_row - margin : first_row, :] = before_ref[0]
    here[:, first_row : first_row + rows, :] = states_ref[0]
    here[:, first_row + rows : first_row + rows + margin, :] = after_ref[0]
    old, new = here, there
    for step in range(STEPS):
        final = step == STEPS - 1
        for t in range(1, last + 1):
            slope = east(old[1, tile(t), :]) + north(old, 2, t)
            height = masked(old[0, tile(t), :] - (0.5 * FLOW_FACTOR) * slope, t)
            new[0, tile(t), :] = height
            if final and 1 < t < last:
                height_ref[0, tile(t - 2), :] = height
        for t in range(2 if final else 1, last if final else last + 1):
            factor = jnp.concatenate([coriolis_ref[tile(t), :]] * (width // LANES), axis=1)
            east_old, north_old = old[1, tile(t), :], old[2, tile(t), :]
            east_new = (
                east_old - (0.5 * PRESSURE_FACTOR) * east(new[0, tile(t), :]) + factor * north_old
            )
            north_new = north_old - (0.5 * PRESSURE_FACTOR) * north(new, 0, t) - factor * east_old
            if final:
                winds_ref[0, 0, tile(t - 2), :] = east_new
                winds_ref[0, 1, tile(t - 2), :] = north_new
            else:
                new[1, tile(t), :] = masked(east_new, t)
                new[2, tile(t), :] = masked(north_new, t)
        old, new = new, old


def forecast(states, before, after, coriolis, band_index, band_count):
    members, fields, rows, width = states.shape
    margin = 2 * STEPS
    frame = rows + 4 * SUBLANES
    factors = lax.dynamic_slice_in_dim(
        jnp.pad(coriolis, (2 * SUBLANES, 2 * SUBLANES)), band_index * rows, frame
    )
    factors = jnp.broadcast_to(factors[:, None], (frame, LANES))
    inside = jnp.stack([band_index > 0, band_index < band_count - 1]).astype(jnp.float32)
    return pl.pallas_call(
        functools.partial(forecast_kernel, margin),
        grid=(members,),
        in_specs=[
            pl.BlockSpec(memory_space=pltpu.SMEM),
            pl.BlockSpec((frame, LANES), lambda m: (0, 0)),
            pl.BlockSpec((1, fields, rows, width), lambda m: (m, 0, 0, 0)),
            pl.BlockSpec((1, fields, margin, width), lambda m: (m, 0, 0, 0)),
            pl.BlockSpec((1, fields, margin, width), lambda m: (m, 0, 0, 0)),
        ],
        out_specs=[
            pl.BlockSpec((1, rows, width), lambda m: (m, 0, 0)),
            pl.BlockSpec((1, fields - 1, rows, width), lambda m: (m, 0, 0, 0)),
        ],
        out_shape=[
            jax.ShapeDtypeStruct((members, rows, width), jnp.float32),
            jax.ShapeDtypeStruct((members, fields - 1, rows, width), jnp.float32),
        ],
        scratch_shapes=[pltpu.VMEM((fields, frame, width), jnp.float32)] * 2,
        cost_estimate=pl.CostEstimate(
            flops=40 * states.size * STEPS, bytes_accessed=8 * states.size, transcendentals=0
        ),
    )(inside, factors, states, before, after)


def tapering(cells, grid_width, block_cells, length):
    longitude = cells.astype(jnp.float32)
    tile_total = grid_width // block_cells
    centre = jnp.arange(tile_total).astype(jnp.float32) * block_cells + 0.5 * (block_cells - 1)
    distance = jnp.abs(longitude[..., :, None] - centre)
    distance = jnp.minimum(distance, grid_width - distance)
    return jnp.exp(-0.5 * (distance / length) ** 2)


def member_weights(heights, cells, values, block_cells, length):
    grid_width = heights.shape[-1]
    chosen_cells = (
        cells[:, None, :] == lax.broadcasted_iota(jnp.int32, (1, grid_width, 1), 1)
    ).astype(jnp.float32)
    observed = jnp.einsum("erl,rlo->reo", heights, chosen_cells, precision=lax.Precision.HIGHEST)
    misfit = (values[:, None, :] - observed) ** 2
    taper_weights = tapering(cells, grid_width, block_cells, length)
    likelihood = (
        -0.5
        / OBSERVATION_VARIANCE
        * jnp.einsum("reo,rob->rbe", misfit, taper_weights, precision=lax.Precision.HIGHEST)
    )
    largest = jnp.max(likelihood, axis=-1, keepdims=True)
    scaled = jnp.exp(likelihood - largest)
    return scaled / jnp.sum(scaled, axis=-1, keepdims=True)


def mixing_matrix(weights, draws):
    member_count = weights.shape[-1]
    split = draws.reshape(draws.shape[:-1] + (3, member_count))
    column = lax.broadcasted_iota(jnp.int32, (1, 1, 1, member_count), 3)
    picks = MERGE_FIRST * (split[:, :, 0, :, None] == column).astype(jnp.float32)
    picks = picks + BLEND_COEF_TWO * (split[:, :, 1, :, None] == column).astype(jnp.float32)
    picks = picks + MERGE_THIRD * (split[:, :, 2, :, None] == column).astype(jnp.float32)
    return (1.0 - RELAXATION) * weights[:, :, None, :] + RELAXATION * picks


def merge_fields(members, mixing, block_cells):
    member_count, fields, count_of_rows, grid_width = members.shape
    blocks = members.reshape(
        member_count, fields, count_of_rows, grid_width // block_cells, block_cells
    )
    updated = jnp.einsum("rbek,kfrbc->efrbc", mixing, blocks, precision=lax.Precision.HIGHEST)
    return updated.reshape(member_count, fields, count_of_rows, grid_width)


def send_all(pieces, axis):
    count = lax.axis_size(axis)
    received = [pieces[0]]
    for d in range(1, count):
        received.append(lax.ppermute(pieces[d], axis, [(i, (i + d) % count) for i in range(count)]))
    return received


def row_pieces(array, axis, dim):
    count = lax.axis_size(axis)
    own = lax.axis_index(axis)
    length = array.shape[dim] // count
    return [
        lax.dynamic_slice_in_dim(array, lax.rem(own + d, count) * length, length, axis=dim)
        for d in range(count)
    ]


def assemble(received, axis, dim):
    count = lax.axis_size(axis)
    own = lax.axis_index(axis)
    length = received[0].shape[dim]
    shape = list(received[0].shape)
    shape[dim] = length * count
    whole = jnp.zeros(shape, received[0].dtype)
    for d, piece in enumerate(received):
        start = lax.rem(own + count - d, count) * length
        whole = lax.dynamic_update_slice_in_dim(whole, piece, start, axis=dim)
    return whole


def relative_draws(draws, axis, members_dev):
    count = lax.axis_size(axis)
    own = lax.axis_index(axis)
    owner = draws // members_dev
    place = lax.rem(own + count - owner, count) * members_dev + draws % members_dev
    split = place.reshape(place.shape[:-1] + (3, count, members_dev))
    doubled = jnp.concatenate([split, split], axis=-2)
    turned = lax.dynamic_slice_in_dim(doubled, own, count, axis=-2)
    return turned.reshape(draws.shape)


def body(particle_states, coriolis, observed_cells, observed_values, resample_draws):
    members_dev, fields, count_of_rows, grid_width = particle_states.shape
    count = lax.axis_size("mem")
    before, after = edge_rows(particle_states, "dom", 2, 2 * STEPS)
    height, winds = forecast(
        particle_states, before, after, coriolis, lax.axis_index("dom"), lax.axis_size("dom")
    )
    cells = observed_cells[0]
    values = observed_values[0]
    draws = relative_draws(resample_draws[0], "mem", members_dev)
    heights = jnp.concatenate(send_all(row_pieces(height, "mem", 1), "mem"), axis=0)
    winds_all = jnp.concatenate(send_all(row_pieces(winds, "mem", 2), "mem"), axis=0)
    weights = member_weights(heights, cells, values, LBLK, LOC)
    mixing = mixing_matrix(weights, draws)

    def hand_back(members):
        updated = merge_fields(members, mixing, LBLK)
        pieces = [updated[d * members_dev : (d + 1) * members_dev] for d in range(count)]
        return assemble(send_all(pieces, "mem"), "mem", 2)

    return jnp.concatenate([hand_back(heights[:, None]), hand_back(winds_all)], axis=1)


def solution(mesh):
    return jax.shard_map(
        body,
        mesh=mesh,
        in_specs=(
            P("mem", None, "dom", None),
            P(),
            P("dom", "mem", None),
            P("dom", "mem", None),
            P("dom", "mem", None, None),
        ),
        out_specs=P("mem", None, "dom", None),
        check_vma=False,
    )
```

```python
import functools

import jax
import jax.numpy as jnp
from jax import lax
from jax.experimental import pallas as pl
from jax.experimental.pallas import tpu as pltpu
from jax.sharding import PartitionSpec as P


LBLK = 128
LOC = 64
STEPS = 2
SUBLANES = 8
LANES = 128
EARLY_MEMBERS = 3


FLOW_FACTOR = 1.0
PRESSURE_FACTOR = 1.0
OBSERVATION_VARIANCE = 16.0
RELAXATION = 0.5
MERGE_FIRST = 0.75
BLEND_COEF_TWO = (13.0**0.5 + 1.0) / 8.0
MERGE_THIRD = -(13.0**0.5 - 1.0) / 8.0


def edge_rows(array, axis, dim, width):
    count, length = (lax.axis_size(axis), array.shape[dim])
    up = [(i, i + 1) for i in range(count - 1)]
    down = [(j, i) for i, j in up]
    before = lax.ppermute(lax.slice_in_dim(array, length - width, length, axis=dim), axis, up)
    after = lax.ppermute(lax.slice_in_dim(array, 0, width, axis=dim), axis, down)
    return before, after


def early_kernel(margin, coriolis_ref, states_ref, all_ref, here, there):
    forecast_steps(margin, None, coriolis_ref, states_ref, None, None,
                   all_ref.at[:, 0], all_ref.at[:, 1:], here, there)


def forecast_steps(margin, inside_ref, coriolis_ref, states_ref, before_ref, after_ref,
                   height_ref, winds_ref, here, there):
    rows, width = states_ref.shape[2:]
    last = rows // SUBLANES + 2
    first_row = 2 * SUBLANES
    with_halo = before_ref is not None

    def tile(t, shift=0):
        return slice(t * SUBLANES + shift, (t + 1) * SUBLANES + shift)

    def east(quantity):
        return pltpu.roll(quantity, width - 1, 1) - pltpu.roll(quantity, 1, 1)

    def north(ref, field, t):
        return ref[field, tile(t, 1), :] - ref[field, tile(t, -1), :]

    def masked(quantity, t):
        if t == 1:
            return quantity * inside_ref[0]
        if t == last:
            return quantity * inside_ref[1]
        return quantity

    here[:, first_row : first_row + rows, :] = states_ref[0]
    if with_halo:
        here[:, first_row - margin : first_row, :] = before_ref[0]
        here[:, first_row + rows : first_row + rows + margin, :] = after_ref[0]
    old, new = here, there
    for step in range(STEPS):
        final = step == STEPS - 1
        for t in range(1, last + 1) if with_halo else range(2, last):
            slope = east(old[1, tile(t), :]) + north(old, 2, t)
            height = masked(old[0, tile(t), :] - (0.5 * FLOW_FACTOR) * slope, t)
            new[0, tile(t), :] = height
            if final and 1 < t < last:
                height_ref[0, tile(t - 2), :] = height
        for t in range(1, last + 1) if with_halo and not final else range(2, last):
            factor = jnp.concatenate([coriolis_ref[tile(t), :]] * (width // LANES), axis=1)
            east_old, north_old = old[1, tile(t), :], old[2, tile(t), :]
            east_new = (
                east_old - (0.5 * PRESSURE_FACTOR) * east(new[0, tile(t), :]) + factor * north_old
            )
            north_new = north_old - (0.5 * PRESSURE_FACTOR) * north(new, 0, t) - factor * east_old
            if final:
                winds_ref[0, 0, tile(t - 2), :] = east_new
                winds_ref[0, 1, tile(t - 2), :] = north_new
            else:
                new[1, tile(t), :] = masked(east_new, t)
                new[2, tile(t), :] = masked(north_new, t)
        old, new = new, old


def coriolis_frame(coriolis, band_index, rows):
    frame = rows + 4 * SUBLANES
    factors = lax.dynamic_slice_in_dim(
        jnp.pad(coriolis, (2 * SUBLANES, 2 * SUBLANES)), band_index * rows, frame
    )
    return jnp.broadcast_to(factors[:, None], (frame, LANES))


def forecast_cost(members, states):
    size = members * states.size // states.shape[0]
    return pl.CostEstimate(flops=40 * size * STEPS, bytes_accessed=8 * size, transcendentals=0)


def early_forecast(states, factors, early):
    fields, rows, width = states.shape[1:]
    return pl.pallas_call(
        functools.partial(early_kernel, 2 * STEPS),
        grid=(early,),
        in_specs=[
            pl.BlockSpec(factors.shape, lambda m: (0, 0)),
            pl.BlockSpec((1, fields, rows, width), lambda m: (m, 0, 0, 0)),
        ],
        out_specs=pl.BlockSpec((1, fields, rows, width), lambda m: (m, 0, 0, 0)),
        out_shape=jax.ShapeDtypeStruct((early, fields, rows, width), jnp.float32),
        scratch_shapes=[pltpu.VMEM((fields, factors.shape[0], width), jnp.float32)] * 2,
        cost_estimate=forecast_cost(early, states),
    )(factors, states)


def forecast(states, before, after, factors, band_index, band_count):
    members, fields, rows, width = states.shape
    margin = 2 * STEPS
    inside = jnp.stack([band_index > 0, band_index < band_count - 1]).astype(jnp.float32)
    return pl.pallas_call(
        functools.partial(forecast_steps, margin),
        grid=(members,),
        in_specs=[
            pl.BlockSpec(memory_space=pltpu.SMEM),
            pl.BlockSpec(factors.shape, lambda m: (0, 0)),
            pl.BlockSpec((1, fields, rows, width), lambda m: (m, 0, 0, 0)),
            pl.BlockSpec((1, fields, margin, width), lambda m: (m, 0, 0, 0)),
            pl.BlockSpec((1, fields, margin, width), lambda m: (m, 0, 0, 0)),
        ],
        out_specs=[
            pl.BlockSpec((1, rows, width), lambda m: (m, 0, 0)),
            pl.BlockSpec((1, fields - 1, rows, width), lambda m: (m, 0, 0, 0)),
        ],
        out_shape=[
            jax.ShapeDtypeStruct((members, rows, width), jnp.float32),
            jax.ShapeDtypeStruct((members, fields - 1, rows, width), jnp.float32),
        ],
        scratch_shapes=[pltpu.VMEM((fields, factors.shape[0], width), jnp.float32)] * 2,
        cost_estimate=forecast_cost(members, states),
    )(inside, factors, states, before, after)


def tapering(cells, grid_width, block_cells, length):
    longitude = cells.astype(jnp.float32)
    tile_total = grid_width // block_cells
    centre = jnp.arange(tile_total).astype(jnp.float32) * block_cells + 0.5 * (block_cells - 1)
    distance = jnp.abs(longitude[..., :, None] - centre)
    distance = jnp.minimum(distance, grid_width - distance)
    return jnp.exp(-0.5 * (distance / length) ** 2)


def member_weights(heights, cells, values, block_cells, length):
    grid_width = heights.shape[-1]
    chosen_cells = (
        cells[:, None, :] == lax.broadcasted_iota(jnp.int32, (1, grid_width, 1), 1)
    ).astype(jnp.float32)
    observed = jnp.einsum("erl,rlo->reo", heights, chosen_cells, precision=lax.Precision.HIGHEST)
    misfit = (values[:, None, :] - observed) ** 2
    taper_weights = tapering(cells, grid_width, block_cells, length)
    likelihood = (
        -0.5
        / OBSERVATION_VARIANCE
        * jnp.einsum("reo,rob->rbe", misfit, taper_weights, precision=lax.Precision.HIGHEST)
    )
    largest = jnp.max(likelihood, axis=-1, keepdims=True)
    scaled = jnp.exp(likelihood - largest)
    return scaled / jnp.sum(scaled, axis=-1, keepdims=True)


def mixing_matrix(weights, draws):
    member_count = weights.shape[-1]
    split = draws.reshape(draws.shape[:-1] + (3, member_count))
    column = lax.broadcasted_iota(jnp.int32, (1, 1, 1, member_count), 3)
    picks = MERGE_FIRST * (split[:, :, 0, :, None] == column).astype(jnp.float32)
    picks = picks + BLEND_COEF_TWO * (split[:, :, 1, :, None] == column).astype(jnp.float32)
    picks = picks + MERGE_THIRD * (split[:, :, 2, :, None] == column).astype(jnp.float32)
    return (1.0 - RELAXATION) * weights[:, :, None, :] + RELAXATION * picks


def merge_fields(members, mixing, block_cells):
    member_count, fields, count_of_rows, grid_width = members.shape
    blocks = members.reshape(
        member_count, fields, count_of_rows, grid_width // block_cells, block_cells
    )
    updated = jnp.einsum("rbek,kfrbc->efrbc", mixing, blocks, precision=lax.Precision.HIGHEST)
    return updated.reshape(member_count, fields, count_of_rows, grid_width)


def shifts(count, d, targets):
    return [(i, (i + d) % count) for i in range(count) if (i + d) % count in targets]


def send_all(pieces, axis, targets=None):
    count = lax.axis_size(axis)
    targets = range(count) if targets is None else targets
    return pieces[:1] + [
        lax.ppermute(pieces[d], axis, shifts(count, d, targets)) for d in range(1, count)
    ]


def row_pieces(array, axis, dim):
    count = lax.axis_size(axis)
    own = lax.axis_index(axis)
    length = array.shape[dim] // count
    pieces = [
        lax.dynamic_slice_in_dim(array, lax.rem(own + d, count) * length, length, axis=dim)
        for d in range(count)
    ]
    return lax.optimization_barrier(pieces)


def put_back(whole, received, axis, field):
    count = lax.axis_size(axis)
    own = lax.axis_index(axis)
    length = received[0].shape[2]
    for d, piece in enumerate(received):
        start = lax.rem(own + count - d, count) * length
        whole = lax.dynamic_update_slice(whole, piece, (0, field, start, 0))
    return whole


def relative_draws(draws, axis, members_dev, early):
    count = lax.axis_size(axis)
    own = lax.axis_index(axis)
    member = draws % members_dev
    distance = lax.rem(own + count - draws // members_dev, count)
    late = members_dev - early
    place = jnp.where(
        member < early,
        distance * early + member,
        count * early + distance * late + member - early,
    )
    split = place.reshape(place.shape[:-1] + (3, count, members_dev))
    doubled = jnp.concatenate([split, split], axis=-2)
    turned = lax.dynamic_slice_in_dim(doubled, own, count, axis=-2)
    return turned.reshape(draws.shape)


def body(particle_states, coriolis, observed_cells, observed_values, resample_draws):
    members_dev, _, count_of_rows, _ = particle_states.shape
    count = lax.axis_size("mem")
    own = lax.axis_index("mem")
    band_index = lax.axis_index("dom")
    margin = 2 * STEPS
    early = EARLY_MEMBERS
    piece = count_of_rows // count
    inner = [
        j for j in range(count)
        if j * piece >= margin and (j + 1) * piece <= count_of_rows - margin
    ]
    outer = [j for j in range(count) if j not in inner]
    factors = coriolis_frame(coriolis, band_index, count_of_rows)

    first = early_forecast(particle_states, factors, early)
    first_pieces = row_pieces(first, "mem", 2)
    first_inner = send_all(first_pieces, "mem", inner)
    states, _ = lax.optimization_barrier((particle_states, first_pieces))
    before, after = edge_rows(states, "dom", 2, margin)
    height, winds = forecast(states, before, after, factors, band_index, lax.axis_size("dom"))
    again = jnp.concatenate([height[:early, None], winds[:early]], axis=1)
    first_outer = send_all(row_pieces(again, "mem", 2), "mem", outer)
    late_heights = send_all(row_pieces(height[early:], "mem", 1), "mem")
    late_winds = send_all(row_pieces(winds[early:], "mem", 2), "mem")
    first_inner, first_outer, late_heights = lax.optimization_barrier(
        (first_inner, first_outer, late_heights)
    )

    is_outer = jnp.any(jnp.stack([own == j for j in outer]))
    firsts = [jnp.where(is_outer, a, b) for a, b in zip(first_outer, first_inner)]
    heights = jnp.concatenate([a[:, 0] for a in firsts] + late_heights, axis=0)
    winds_all = jnp.concatenate([a[:, 1:] for a in firsts] + late_winds, axis=0)

    cells = observed_cells[0]
    values = observed_values[0]
    draws = relative_draws(resample_draws[0], "mem", members_dev, early)
    weights = member_weights(heights, cells, values, LBLK, LOC)
    mixing = mixing_matrix(weights, draws)

    def hand_back(members):
        updated = merge_fields(members, mixing, LBLK)
        pieces = [updated[d * members_dev : (d + 1) * members_dev] for d in range(count)]
        return send_all(pieces, "mem")

    analysed = jnp.zeros(particle_states.shape, particle_states.dtype)
    analysed = put_back(analysed, hand_back(heights[:, None]), "mem", 0)
    return put_back(analysed, hand_back(winds_all), "mem", 1)


def solution(mesh):
    return jax.shard_map(
        body,
        mesh=mesh,
        in_specs=(
            P("mem", None, "dom", None),
            P(),
            P("dom", "mem", None),
            P("dom", "mem", None),
            P("dom", "mem", None, None),
        ),
        out_specs=P("mem", None, "dom", None),
        check_vma=False,
    )
```

```python
import functools

import jax
import jax.numpy as jnp
from jax import lax
from jax.experimental import pallas as pl
from jax.experimental.pallas import tpu as pltpu
from jax.sharding import PartitionSpec as P


LBLK = 128
LOC = 64
STEPS = 2
SUBLANES = 8
LANES = 128


FLOW_FACTOR = 1.0
PRESSURE_FACTOR = 1.0
OBSERVATION_VARIANCE = 16.0
RELAXATION = 0.5
MERGE_FIRST = 0.75
BLEND_COEF_TWO = (13.0**0.5 + 1.0) / 8.0
MERGE_THIRD = -(13.0**0.5 - 1.0) / 8.0


def edge_rows(array, axis, dim, width):
    count, length = (lax.axis_size(axis), array.shape[dim])
    up = [(i, i + 1) for i in range(count - 1)]
    down = [(j, i) for i, j in up]
    before = lax.ppermute(lax.slice_in_dim(array, length - width, length, axis=dim), axis, up)
    after = lax.ppermute(lax.slice_in_dim(array, 0, width, axis=dim), axis, down)
    return before, after


def early_kernel(margin, coriolis_ref, states_ref, height_ref, here, there):
    forecast_steps(margin, None, coriolis_ref, states_ref, None, None, height_ref, None, here, there)


def forecast_steps(margin, inside_ref, coriolis_ref, states_ref, before_ref, after_ref,
                   height_ref, winds_ref, here, there):
    rows, width = states_ref.shape[2:]
    last = rows // SUBLANES + 2
    first_row = 2 * SUBLANES
    with_halo = before_ref is not None

    def tile(t, shift=0):
        return slice(t * SUBLANES + shift, (t + 1) * SUBLANES + shift)

    def east(quantity):
        return pltpu.roll(quantity, width - 1, 1) - pltpu.roll(quantity, 1, 1)

    def north(ref, field, t):
        return ref[field, tile(t, 1), :] - ref[field, tile(t, -1), :]

    def masked(quantity, t):
        if t == 1:
            return quantity * inside_ref[0]
        if t == last:
            return quantity * inside_ref[1]
        return quantity

    here[:, first_row : first_row + rows, :] = states_ref[0]
    if with_halo:
        here[:, first_row - margin : first_row, :] = before_ref[0]
        here[:, first_row + rows : first_row + rows + margin, :] = after_ref[0]
    old, new = here, there
    for step in range(STEPS):
        final = step == STEPS - 1
        for t in range(1, last + 1) if with_halo else range(2, last):
            slope = east(old[1, tile(t), :]) + north(old, 2, t)
            height = masked(old[0, tile(t), :] - (0.5 * FLOW_FACTOR) * slope, t)
            new[0, tile(t), :] = height
            if final and 1 < t < last:
                height_ref[0, tile(t - 2), :] = height
        if final and winds_ref is None:
            break
        for t in range(1, last + 1) if with_halo and not final else range(2, last):
            factor = jnp.concatenate([coriolis_ref[tile(t), :]] * (width // LANES), axis=1)
            east_old, north_old = old[1, tile(t), :], old[2, tile(t), :]
            east_new = (
                east_old - (0.5 * PRESSURE_FACTOR) * east(new[0, tile(t), :]) + factor * north_old
            )
            north_new = north_old - (0.5 * PRESSURE_FACTOR) * north(new, 0, t) - factor * east_old
            if final:
                winds_ref[0, 0, tile(t - 2), :] = east_new
                winds_ref[0, 1, tile(t - 2), :] = north_new
            else:
                new[1, tile(t), :] = masked(east_new, t)
                new[2, tile(t), :] = masked(north_new, t)
        old, new = new, old


def coriolis_frame(coriolis, band_index, rows):
    frame = rows + 4 * SUBLANES
    factors = lax.dynamic_slice_in_dim(
        jnp.pad(coriolis, (2 * SUBLANES, 2 * SUBLANES)), band_index * rows, frame
    )
    return jnp.broadcast_to(factors[:, None], (frame, LANES))


def forecast_cost(states):
    return pl.CostEstimate(
        flops=40 * states.size * STEPS, bytes_accessed=8 * states.size, transcendentals=0
    )


def early_heights(states, factors):
    members, fields, rows, width = states.shape
    return pl.pallas_call(
        functools.partial(early_kernel, 2 * STEPS),
        grid=(members,),
        in_specs=[
            pl.BlockSpec(factors.shape, lambda m: (0, 0)),
            pl.BlockSpec((1, fields, rows, width), lambda m: (m, 0, 0, 0)),
        ],
        out_specs=pl.BlockSpec((1, rows, width), lambda m: (m, 0, 0)),
        out_shape=jax.ShapeDtypeStruct((members, rows, width), jnp.float32),
        scratch_shapes=[pltpu.VMEM((fields, factors.shape[0], width), jnp.float32)] * 2,
        cost_estimate=forecast_cost(states),
    )(factors, states)


def forecast(states, before, after, factors, band_index, band_count):
    members, fields, rows, width = states.shape
    margin = 2 * STEPS
    inside = jnp.stack([band_index > 0, band_index < band_count - 1]).astype(jnp.float32)
    return pl.pallas_call(
        functools.partial(forecast_steps, margin),
        grid=(members,),
        in_specs=[
            pl.BlockSpec(memory_space=pltpu.SMEM),
            pl.BlockSpec(factors.shape, lambda m: (0, 0)),
            pl.BlockSpec((1, fields, rows, width), lambda m: (m, 0, 0, 0)),
            pl.BlockSpec((1, fields, margin, width), lambda m: (m, 0, 0, 0)),
            pl.BlockSpec((1, fields, margin, width), lambda m: (m, 0, 0, 0)),
        ],
        out_specs=[
            pl.BlockSpec((1, rows, width), lambda m: (m, 0, 0)),
            pl.BlockSpec((1, fields - 1, rows, width), lambda m: (m, 0, 0, 0)),
        ],
        out_shape=[
            jax.ShapeDtypeStruct((members, rows, width), jnp.float32),
            jax.ShapeDtypeStruct((members, fields - 1, rows, width), jnp.float32),
        ],
        scratch_shapes=[pltpu.VMEM((fields, factors.shape[0], width), jnp.float32)] * 2,
        cost_estimate=forecast_cost(states),
    )(inside, factors, states, before, after)


def tapering(cells, grid_width, block_cells, length):
    longitude = cells.astype(jnp.float32)
    tile_total = grid_width // block_cells
    centre = jnp.arange(tile_total).astype(jnp.float32) * block_cells + 0.5 * (block_cells - 1)
    distance = jnp.abs(longitude[..., :, None] - centre)
    distance = jnp.minimum(distance, grid_width - distance)
    return jnp.exp(-0.5 * (distance / length) ** 2)


def member_weights(heights, cells, values, block_cells, length):
    grid_width = heights.shape[-1]
    chosen_cells = (
        cells[:, None, :] == lax.broadcasted_iota(jnp.int32, (1, grid_width, 1), 1)
    ).astype(jnp.float32)
    observed = jnp.einsum("erl,rlo->reo", heights, chosen_cells, precision=lax.Precision.HIGHEST)
    misfit = (values[:, None, :] - observed) ** 2
    taper_weights = tapering(cells, grid_width, block_cells, length)
    likelihood = (
        -0.5
        / OBSERVATION_VARIANCE
        * jnp.einsum("reo,rob->rbe", misfit, taper_weights, precision=lax.Precision.HIGHEST)
    )
    largest = jnp.max(likelihood, axis=-1, keepdims=True)
    scaled = jnp.exp(likelihood - largest)
    return scaled / jnp.sum(scaled, axis=-1, keepdims=True)


def mixing_matrix(weights, draws):
    member_count = weights.shape[-1]
    split = draws.reshape(draws.shape[:-1] + (3, member_count))
    column = lax.broadcasted_iota(jnp.int32, (1, 1, 1, member_count), 3)
    picks = MERGE_FIRST * (split[:, :, 0, :, None] == column).astype(jnp.float32)
    picks = picks + BLEND_COEF_TWO * (split[:, :, 1, :, None] == column).astype(jnp.float32)
    picks = picks + MERGE_THIRD * (split[:, :, 2, :, None] == column).astype(jnp.float32)
    return (1.0 - RELAXATION) * weights[:, :, None, :] + RELAXATION * picks


def merge_fields(members, mixing, block_cells):
    member_count, fields, count_of_rows, grid_width = members.shape
    blocks = members.reshape(
        member_count, fields, count_of_rows, grid_width // block_cells, block_cells
    )
    updated = jnp.einsum("rbek,kfrbc->efrbc", mixing, blocks, precision=lax.Precision.HIGHEST)
    return updated.reshape(member_count, fields, count_of_rows, grid_width)


def shifts(count, d, targets):
    return [(i, (i + d) % count) for i in range(count) if (i + d) % count in targets]


def send_all(pieces, axis, targets=None):
    count = lax.axis_size(axis)
    targets = range(count) if targets is None else targets
    return pieces[:1] + [
        lax.ppermute(pieces[d], axis, shifts(count, d, targets)) for d in range(1, count)
    ]


def row_pieces(array, axis, dim):
    count = lax.axis_size(axis)
    own = lax.axis_index(axis)
    length = array.shape[dim] // count
    pieces = [
        lax.dynamic_slice_in_dim(array, lax.rem(own + d, count) * length, length, axis=dim)
        for d in range(count)
    ]
    return lax.optimization_barrier(pieces)


def put_back(whole, received, axis, field):
    count = lax.axis_size(axis)
    own = lax.axis_index(axis)
    length = received[0].shape[2]
    for d, piece in enumerate(received):
        start = lax.rem(own + count - d, count) * length
        whole = lax.dynamic_update_slice(whole, piece, (0, field, start, 0))
    return whole


def relative_draws(draws, axis, members_dev):
    count = lax.axis_size(axis)
    own = lax.axis_index(axis)
    distance = lax.rem(own + count - draws // members_dev, count)
    place = distance * members_dev + draws % members_dev
    split = place.reshape(place.shape[:-1] + (3, count, members_dev))
    doubled = jnp.concatenate([split, split], axis=-2)
    turned = lax.dynamic_slice_in_dim(doubled, own, count, axis=-2)
    return turned.reshape(draws.shape)


def body(particle_states, coriolis, observed_cells, observed_values, resample_draws):
    members_dev, _, count_of_rows, _ = particle_states.shape
    count = lax.axis_size("mem")
    own = lax.axis_index("mem")
    band_index = lax.axis_index("dom")
    margin = 2 * STEPS
    piece = count_of_rows // count
    inner = [
        j for j in range(count)
        if j * piece >= margin and (j + 1) * piece <= count_of_rows - margin
    ]
    outer = [j for j in range(count) if j not in inner]
    factors = coriolis_frame(coriolis, band_index, count_of_rows)

    first = row_pieces(early_heights(particle_states, factors), "mem", 1)
    inner_heights = send_all(first, "mem", inner)
    states, _ = lax.optimization_barrier((particle_states, first))
    before, after = edge_rows(states, "dom", 2, margin)
    height, winds = forecast(states, before, after, factors, band_index, lax.axis_size("dom"))
    outer_heights = send_all(row_pieces(height, "mem", 1), "mem", outer)
    winds_all = send_all(row_pieces(winds, "mem", 2), "mem")
    inner_heights, outer_heights = lax.optimization_barrier((inner_heights, outer_heights))
    is_outer = jnp.any(jnp.stack([own == j for j in outer]))
    heights = jnp.concatenate(
        [jnp.where(is_outer, a, b) for a, b in zip(outer_heights, inner_heights)], axis=0
    )
    winds_all = jnp.concatenate(winds_all, axis=0)

    cells = observed_cells[0]
    values = observed_values[0]
    draws = relative_draws(resample_draws[0], "mem", members_dev)
    weights = member_weights(heights, cells, values, LBLK, LOC)
    mixing = mixing_matrix(weights, draws)

    def hand_back(members):
        updated = merge_fields(members, mixing, LBLK)
        pieces = [updated[d * members_dev : (d + 1) * members_dev] for d in range(count)]
        return send_all(pieces, "mem")

    analysed = jnp.zeros(particle_states.shape, particle_states.dtype)
    analysed = put_back(analysed, hand_back(heights[:, None]), "mem", 0)
    return put_back(analysed, hand_back(winds_all), "mem", 1)


def solution(mesh):
    return jax.shard_map(
        body,
        mesh=mesh,
        in_specs=(
            P("mem", None, "dom", None),
            P(),
            P("dom", "mem", None),
            P("dom", "mem", None),
            P("dom", "mem", None, None),
        ),
        out_specs=P("mem", None, "dom", None),
        check_vma=False,
    )
```

```python
import functools

import jax
import jax.numpy as jnp
from jax import lax
from jax.experimental import pallas as pl
from jax.experimental.pallas import tpu as pltpu
from jax.sharding import PartitionSpec as P


LBLK = 128
LOC = 64
STEPS = 2
SUBLANES = 8
LANES = 128


FLOW_FACTOR = 1.0
PRESSURE_FACTOR = 1.0
OBSERVATION_VARIANCE = 16.0
RELAXATION = 0.5
MERGE_FIRST = 0.75
BLEND_COEF_TWO = (13.0**0.5 + 1.0) / 8.0
MERGE_THIRD = -(13.0**0.5 - 1.0) / 8.0


def edge_rows(array, axis, dim, width):
    count, length = (lax.axis_size(axis), array.shape[dim])
    up = [(i, i + 1) for i in range(count - 1)]
    down = [(j, i) for i, j in up]
    before = lax.ppermute(lax.slice_in_dim(array, length - width, length, axis=dim), axis, up)
    after = lax.ppermute(lax.slice_in_dim(array, 0, width, axis=dim), axis, down)
    return before, after


def forecast_steps(here, there, tiles, final, masked, factor):
    width = here.shape[2]

    def tile(t, shift=0):
        return slice(t * SUBLANES + shift, (t + 1) * SUBLANES + shift)

    def east(quantity):
        return pltpu.roll(quantity, width - 1, 1) - pltpu.roll(quantity, 1, 1)

    def north(ref, field, t):
        return ref[field, tile(t, 1), :] - ref[field, tile(t, -1), :]

    old, new = here, there
    for step in range(STEPS):
        for t in tiles:
            slope = east(old[1, tile(t), :]) + north(old, 2, t)
            new[0, tile(t), :] = masked(
                old[0, tile(t), :] - (0.5 * FLOW_FACTOR) * slope, t
            )
        for t in final if step == STEPS - 1 else tiles:
            turn = factor(t)
            east_old, north_old = old[1, tile(t), :], old[2, tile(t), :]
            east_new = (
                east_old - (0.5 * PRESSURE_FACTOR) * east(new[0, tile(t), :]) + turn * north_old
            )
            north_new = north_old - (0.5 * PRESSURE_FACTOR) * north(new, 0, t) - turn * east_old
            new[1, tile(t), :] = masked(east_new, t)
            new[2, tile(t), :] = masked(north_new, t)
        old, new = new, old
    return old


def coriolis_tile(coriolis_ref, t, width):
    factors = coriolis_ref[t * SUBLANES : (t + 1) * SUBLANES, :]
    return jnp.concatenate([factors] * (width // LANES), axis=1)


def early_kernel(count, place_ref, coriolis_ref, states_ref, *refs):
    rows, width = states_ref.shape[2:]
    outs, (here, there) = refs[:-2], refs[-2:]
    first = 2 * SUBLANES
    tiles = range(2, rows // SUBLANES + 2)
    here[:, first : first + rows, :] = states_ref[0]
    done = forecast_steps(
        here, there, tiles, tiles,
        lambda quantity, t: quantity,
        lambda t: coriolis_tile(coriolis_ref, t, width),
    )
    if len(outs) == 2:
        outs[0][0] = done[0, first : first + rows, :]
        outs[1][0] = done[1:, first : first + rows, :]
        return
    piece = rows // count
    for d in range(count):
        start = pl.multiple_of(lax.rem(place_ref[0] + d, count) * piece, SUBLANES)
        outs[d][0] = done[0, pl.ds(first + start, piece), :]
        outs[count + d][0] = done[1:, pl.ds(first + start, piece), :]


def edge_kernel(inside_ref, coriolis_ref, low_ref, high_ref, before_ref, after_ref,
                height_ref, winds_ref, here, there):
    margin, width = before_ref.shape[2:]
    last_tile = coriolis_ref.shape[0] // SUBLANES - 5
    for edge in range(2):
        if edge == 0:
            here[:, 2 * SUBLANES - margin : 2 * SUBLANES, :] = before_ref[0]
            here[:, 2 * SUBLANES : 4 * SUBLANES, :] = low_ref[0]
        else:
            here[:, SUBLANES : 3 * SUBLANES, :] = high_ref[0]
            here[:, 3 * SUBLANES : 3 * SUBLANES + margin, :] = after_ref[0]
        outside = 1 if edge == 0 else 3
        shift = 0 if edge == 0 else last_tile
        done = forecast_steps(
            here, there, (1, 2, 3), (2,),
            lambda quantity, t: quantity * inside_ref[edge] if t == outside else quantity,
            lambda t: coriolis_tile(coriolis_ref, t + shift, width),
        )
        rows = slice(edge * SUBLANES, (edge + 1) * SUBLANES)
        height_ref[0, rows, :] = done[0, 2 * SUBLANES : 3 * SUBLANES, :]
        winds_ref[0, :, rows, :] = done[1:, 2 * SUBLANES : 3 * SUBLANES, :]


def coriolis_frame(coriolis, band_index, rows):
    padded = jnp.pad(coriolis, (2 * SUBLANES, 2 * SUBLANES))
    spread = jnp.broadcast_to(padded[:, None], padded.shape + (LANES,))
    return lax.dynamic_slice_in_dim(spread, band_index * rows, rows + 4 * SUBLANES)


def forecast_cost(states, rows):
    size = states.size * rows // states.shape[2]
    return pl.CostEstimate(flops=40 * size * STEPS, bytes_accessed=8 * size, transcendentals=0)


def early_pieces(states, factors, axis):
    members, fields, rows, width = states.shape
    count = lax.axis_size(axis)
    piece = rows // count
    whole = piece % SUBLANES != 0
    heights, winds = (rows,) if whole else (piece,) * count, (rows,) if whole else (piece,) * count
    place = lax.axis_index(axis).astype(jnp.int32).reshape(1)
    found = pl.pallas_call(
        functools.partial(early_kernel, count),
        grid=(members,),
        in_specs=[
            pl.BlockSpec(memory_space=pltpu.SMEM),
            pl.BlockSpec(factors.shape, lambda m: (0, 0)),
            pl.BlockSpec((1, fields, rows, width), lambda m: (m, 0, 0, 0)),
        ],
        out_specs=[pl.BlockSpec((1, r, width), lambda m: (m, 0, 0)) for r in heights]
        + [pl.BlockSpec((1, fields - 1, r, width), lambda m: (m, 0, 0, 0)) for r in winds],
        out_shape=[jax.ShapeDtypeStruct((members, r, width), jnp.float32) for r in heights]
        + [jax.ShapeDtypeStruct((members, fields - 1, r, width), jnp.float32) for r in winds],
        scratch_shapes=[pltpu.VMEM((fields, factors.shape[0], width), jnp.float32)] * 2,
        cost_estimate=forecast_cost(states, rows),
    )(place, factors, states)
    if whole:
        return row_pieces(found[0], axis, 1), row_pieces(found[1], axis, 2)
    return list(found[:count]), list(found[count:])


def edge_forecast(states, before, after, factors, band_index, band_count):
    members, fields, rows, width = states.shape
    margin = 2 * STEPS
    inside = jnp.stack([band_index > 0, band_index < band_count - 1]).astype(jnp.float32)
    last = rows // (2 * SUBLANES) - 1
    return pl.pallas_call(
        edge_kernel,
        grid=(members,),
        in_specs=[
            pl.BlockSpec(memory_space=pltpu.SMEM),
            pl.BlockSpec(factors.shape, lambda m: (0, 0)),
            pl.BlockSpec((1, fields, 2 * SUBLANES, width), lambda m: (m, 0, 0, 0)),
            pl.BlockSpec((1, fields, 2 * SUBLANES, width), lambda m: (m, 0, last, 0)),
            pl.BlockSpec((1, fields, margin, width), lambda m: (m, 0, 0, 0)),
            pl.BlockSpec((1, fields, margin, width), lambda m: (m, 0, 0, 0)),
        ],
        out_specs=[
            pl.BlockSpec((1, 2 * SUBLANES, width), lambda m: (m, 0, 0)),
            pl.BlockSpec((1, fields - 1, 2 * SUBLANES, width), lambda m: (m, 0, 0, 0)),
        ],
        out_shape=[
            jax.ShapeDtypeStruct((members, 2 * SUBLANES, width), jnp.float32),
            jax.ShapeDtypeStruct((members, fields - 1, 2 * SUBLANES, width), jnp.float32),
        ],
        scratch_shapes=[pltpu.VMEM((fields, 5 * SUBLANES, width), jnp.float32)] * 2,
        cost_estimate=forecast_cost(states, 6 * SUBLANES),
    )(inside, factors, states, states, before, after)


def tapering(cells, grid_width, block_cells, length):
    longitude = cells.astype(jnp.float32)
    tile_total = grid_width // block_cells
    centre = jnp.arange(tile_total).astype(jnp.float32) * block_cells + 0.5 * (block_cells - 1)
    distance = jnp.abs(longitude[..., :, None] - centre)
    distance = jnp.minimum(distance, grid_width - distance)
    return jnp.exp(-0.5 * (distance / length) ** 2)


def member_weights(heights, cells, values, block_cells, length):
    grid_width = heights.shape[-1]
    chosen_cells = (
        cells[:, None, :] == lax.broadcasted_iota(jnp.int32, (1, grid_width, 1), 1)
    ).astype(jnp.float32)
    observed = jnp.einsum("erl,rlo->reo", heights, chosen_cells, precision=lax.Precision.HIGHEST)
    misfit = (values[:, None, :] - observed) ** 2
    taper_weights = tapering(cells, grid_width, block_cells, length)
    likelihood = (
        -0.5
        / OBSERVATION_VARIANCE
        * jnp.einsum("reo,rob->rbe", misfit, taper_weights, precision=lax.Precision.HIGHEST)
    )
    largest = jnp.max(likelihood, axis=-1, keepdims=True)
    scaled = jnp.exp(likelihood - largest)
    return scaled / jnp.sum(scaled, axis=-1, keepdims=True)


def mixing_matrix(weights, draws):
    member_count = weights.shape[-1]
    split = draws.reshape(draws.shape[:-1] + (3, member_count))
    column = lax.broadcasted_iota(jnp.int32, (1, 1, 1, member_count), 3)
    picks = MERGE_FIRST * (split[:, :, 0, :, None] == column).astype(jnp.float32)
    picks = picks + BLEND_COEF_TWO * (split[:, :, 1, :, None] == column).astype(jnp.float32)
    picks = picks + MERGE_THIRD * (split[:, :, 2, :, None] == column).astype(jnp.float32)
    return (1.0 - RELAXATION) * weights[:, :, None, :] + RELAXATION * picks


def merge_fields(members, mixing, block_cells):
    member_count, fields, count_of_rows, grid_width = members.shape
    blocks = members.reshape(
        member_count, fields, count_of_rows, grid_width // block_cells, block_cells
    )
    updated = jnp.einsum("rbek,kfrbc->efrbc", mixing, blocks, precision=lax.Precision.HIGHEST)
    return updated.reshape(member_count, fields, count_of_rows, grid_width)


def shifts(count, d, targets):
    return [(i, (i + d) % count) for i in range(count) if (i + d) % count in targets]


def by_reach(count):
    return sorted(range(1, count), key=lambda d: abs(2 * d - count))


def send_all(pieces, axis, targets=None):
    count = lax.axis_size(axis)
    targets = range(count) if targets is None else targets
    received = {0: pieces[0]}
    for d in by_reach(count):
        received[d] = lax.ppermute(pieces[d], axis, shifts(count, d, targets))
    return [received[d] for d in range(count)]


def row_pieces(array, axis, dim):
    count = lax.axis_size(axis)
    own = lax.axis_index(axis)
    length = array.shape[dim] // count
    pieces = [
        lax.dynamic_slice_in_dim(array, lax.rem(own + d, count) * length, length, axis=dim)
        for d in range(count)
    ]
    return lax.optimization_barrier(pieces)


def edge_pieces(array, axis, dim, length):
    count = lax.axis_size(axis)
    own = lax.axis_index(axis)
    held = array.shape[dim]
    pieces = []
    for d in range(count):
        owner = lax.rem(own + d, count)
        start = jnp.where(2 * owner < count, owner * length, held - (count - owner) * length)
        pieces.append(lax.dynamic_slice_in_dim(array, start, length, axis=dim))
    return lax.optimization_barrier(pieces)


def put_back(whole, received, axis, field):
    count = lax.axis_size(axis)
    own = lax.axis_index(axis)
    length = received[0].shape[2]
    for d, piece in enumerate(received):
        start = lax.rem(own + count - d, count) * length
        whole = lax.dynamic_update_slice(whole, piece, (0, field, start, 0))
    return whole


def relative_draws(draws, axis, members_dev):
    count = lax.axis_size(axis)
    own = lax.axis_index(axis)
    distance = lax.rem(own + count - draws // members_dev, count)
    place = distance * members_dev + draws % members_dev
    split = place.reshape(place.shape[:-1] + (3, count, members_dev))
    doubled = jnp.concatenate([split, split], axis=-2)
    turned = lax.dynamic_slice_in_dim(doubled, own, count, axis=-2)
    return turned.reshape(draws.shape)


def body(particle_states, coriolis, observed_cells, observed_values, resample_draws):
    members_dev, _, count_of_rows, _ = particle_states.shape
    count = lax.axis_size("mem")
    own = lax.axis_index("mem")
    band_index = lax.axis_index("dom")
    margin = 2 * STEPS
    piece = count_of_rows // count
    inner = [
        j for j in range(count)
        if j * piece >= margin and (j + 1) * piece <= count_of_rows - margin
    ]
    outer = [j for j in range(count) if j not in inner]
    factors = coriolis_frame(coriolis, band_index, count_of_rows)

    heights, winds = early_pieces(particle_states, factors, "mem")
    inner_heights = send_all(heights, "mem", inner)
    states, heights = lax.optimization_barrier((particle_states, heights))
    before, after = edge_rows(states, "dom", 2, margin)
    inner_winds = send_all(winds, "mem", inner)
    edges = edge_forecast(
        states, before, after, factors, band_index, lax.axis_size("dom")
    )
    outer_heights = send_all(edge_pieces(edges[0], "mem", 1, piece), "mem", outer)
    outer_winds = send_all(edge_pieces(edges[1], "mem", 2, piece), "mem", outer)
    inner_heights, outer_heights = lax.optimization_barrier((inner_heights, outer_heights))
    is_outer = jnp.any(jnp.stack([own == j for j in outer]))

    def gather(at_edge, within):
        return jnp.concatenate(
            [jnp.where(is_outer, a, b) for a, b in zip(at_edge, within)], axis=0
        )

    heights = gather(outer_heights, inner_heights)
    winds_all = gather(outer_winds, inner_winds)

    cells = observed_cells[0]
    values = observed_values[0]
    draws = relative_draws(resample_draws[0], "mem", members_dev)
    weights = member_weights(heights, cells, values, LBLK, LOC)
    mixing = mixing_matrix(weights, draws)

    def hand_back(members):
        updated = merge_fields(members, mixing, LBLK)
        pieces = [updated[d * members_dev : (d + 1) * members_dev] for d in range(count)]
        return send_all(pieces, "mem")

    analysed = jnp.zeros(particle_states.shape, particle_states.dtype)
    analysed = put_back(analysed, hand_back(heights[:, None]), "mem", 0)
    return put_back(analysed, hand_back(winds_all), "mem", 1)


def solution(mesh):
    return jax.shard_map(
        body,
        mesh=mesh,
        in_specs=(
            P("mem", None, "dom", None),
            P(),
            P("dom", "mem", None),
            P("dom", "mem", None),
            P("dom", "mem", None, None),
        ),
        out_specs=P("mem", None, "dom", None),
        check_vma=False,
    )
```

```python
import functools

import jax
import jax.numpy as jnp
from jax import lax
from jax.experimental import pallas as pl
from jax.experimental.pallas import tpu as pltpu
from jax.sharding import PartitionSpec as P


LBLK = 128
LOC = 64
STEPS = 2
SUBLANES = 8
LANES = 128


FLOW_FACTOR = 1.0
PRESSURE_FACTOR = 1.0
OBSERVATION_VARIANCE = 16.0
RELAXATION = 0.5
MERGE_FIRST = 0.75
BLEND_COEF_TWO = (13.0**0.5 + 1.0) / 8.0
MERGE_THIRD = -(13.0**0.5 - 1.0) / 8.0


def edge_rows(array, axis, dim, width):
    count, length = (lax.axis_size(axis), array.shape[dim])
    up = [(i, i + 1) for i in range(count - 1)]
    down = [(j, i) for i, j in up]
    before = lax.ppermute(lax.slice_in_dim(array, length - width, length, axis=dim), axis, up)
    after = lax.ppermute(lax.slice_in_dim(array, 0, width, axis=dim), axis, down)
    return before, after


def forecast_steps(here, there, tiles, final, masked, factor):
    width = here.shape[2]

    def tile(t, shift=0):
        return slice(t * SUBLANES + shift, (t + 1) * SUBLANES + shift)

    def east(quantity):
        return pltpu.roll(quantity, width - 1, 1) - pltpu.roll(quantity, 1, 1)

    def north(ref, field, t):
        return ref[field, tile(t, 1), :] - ref[field, tile(t, -1), :]

    old, new = here, there
    for step in range(STEPS):
        for t in tiles:
            slope = east(old[1, tile(t), :]) + north(old, 2, t)
            new[0, tile(t), :] = masked(
                old[0, tile(t), :] - (0.5 * FLOW_FACTOR) * slope, t
            )
        for t in final if step == STEPS - 1 else tiles:
            turn = factor(t)
            east_old, north_old = old[1, tile(t), :], old[2, tile(t), :]
            east_new = (
                east_old - (0.5 * PRESSURE_FACTOR) * east(new[0, tile(t), :]) + turn * north_old
            )
            north_new = north_old - (0.5 * PRESSURE_FACTOR) * north(new, 0, t) - turn * east_old
            new[1, tile(t), :] = masked(east_new, t)
            new[2, tile(t), :] = masked(north_new, t)
        old, new = new, old
    return old


def coriolis_tile(coriolis_ref, t, width):
    factors = coriolis_ref[t * SUBLANES : (t + 1) * SUBLANES, :]
    return jnp.concatenate([factors] * (width // LANES), axis=1)


def early_kernel(count, place_ref, coriolis_ref, states_ref, *refs):
    rows, width = states_ref.shape[2:]
    outs, (here, there) = refs[:-2], refs[-2:]
    first = 2 * SUBLANES
    tiles = range(2, rows // SUBLANES + 2)
    here[:, first : first + rows, :] = states_ref[0]
    done = forecast_steps(
        here, there, tiles, tiles,
        lambda quantity, t: quantity,
        lambda t: coriolis_tile(coriolis_ref, t, width),
    )
    if len(outs) == 2:
        outs[0][0] = done[0, first : first + rows, :]
        outs[1][0] = done[1:, first : first + rows, :]
        return
    piece = rows // count
    for d in range(count):
        start = pl.multiple_of(lax.rem(place_ref[0] + d, count) * piece, SUBLANES)
        outs[d][0] = done[0, pl.ds(first + start, piece), :]
        outs[count + d][0] = done[1:, pl.ds(first + start, piece), :]


def edge_kernel(inside_ref, coriolis_ref, low_ref, high_ref, before_ref, after_ref,
                height_ref, winds_ref, here, there):
    margin, width = before_ref.shape[2:]
    last_tile = coriolis_ref.shape[0] // SUBLANES - 5
    for edge in range(2):
        if edge == 0:
            here[:, 2 * SUBLANES - margin : 2 * SUBLANES, :] = before_ref[0]
            here[:, 2 * SUBLANES : 4 * SUBLANES, :] = low_ref[0]
        else:
            here[:, SUBLANES : 3 * SUBLANES, :] = high_ref[0]
            here[:, 3 * SUBLANES : 3 * SUBLANES + margin, :] = after_ref[0]
        outside = 1 if edge == 0 else 3
        shift = 0 if edge == 0 else last_tile
        done = forecast_steps(
            here, there, (1, 2, 3), (2,),
            lambda quantity, t: quantity * inside_ref[edge] if t == outside else quantity,
            lambda t: coriolis_tile(coriolis_ref, t + shift, width),
        )
        rows = slice(edge * SUBLANES, (edge + 1) * SUBLANES)
        height_ref[0, rows, :] = done[0, 2 * SUBLANES : 3 * SUBLANES, :]
        winds_ref[0, :, rows, :] = done[1:, 2 * SUBLANES : 3 * SUBLANES, :]


def coriolis_frame(coriolis, band_index, rows):
    padded = jnp.pad(coriolis, (2 * SUBLANES, 2 * SUBLANES))
    spread = jnp.broadcast_to(padded[:, None], padded.shape + (LANES,))
    return lax.dynamic_slice_in_dim(spread, band_index * rows, rows + 4 * SUBLANES)


def forecast_cost(states, rows):
    size = states.size * rows // states.shape[2]
    return pl.CostEstimate(flops=40 * size * STEPS, bytes_accessed=8 * size, transcendentals=0)


def early_pieces(states, factors, axis):
    members, fields, rows, width = states.shape
    count = lax.axis_size(axis)
    piece = rows // count
    whole = piece % SUBLANES != 0
    heights, winds = (rows,) if whole else (piece,) * count, (rows,) if whole else (piece,) * count
    place = lax.axis_index(axis).astype(jnp.int32).reshape(1)
    found = pl.pallas_call(
        functools.partial(early_kernel, count),
        grid=(members,),
        in_specs=[
            pl.BlockSpec(memory_space=pltpu.SMEM),
            pl.BlockSpec(factors.shape, lambda m: (0, 0)),
            pl.BlockSpec((1, fields, rows, width), lambda m: (m, 0, 0, 0)),
        ],
        out_specs=[pl.BlockSpec((1, r, width), lambda m: (m, 0, 0)) for r in heights]
        + [pl.BlockSpec((1, fields - 1, r, width), lambda m: (m, 0, 0, 0)) for r in winds],
        out_shape=[jax.ShapeDtypeStruct((members, r, width), jnp.float32) for r in heights]
        + [jax.ShapeDtypeStruct((members, fields - 1, r, width), jnp.float32) for r in winds],
        scratch_shapes=[pltpu.VMEM((fields, factors.shape[0], width), jnp.float32)] * 2,
        cost_estimate=forecast_cost(states, rows),
    )(place, factors, states)
    if whole:
        return row_pieces(found[0], axis, 1), row_pieces(found[1], axis, 2)
    return list(found[:count]), list(found[count:])


def edge_forecast(states, before, after, factors, band_index, band_count):
    members, fields, rows, width = states.shape
    margin = 2 * STEPS
    inside = jnp.stack([band_index > 0, band_index < band_count - 1]).astype(jnp.float32)
    last = rows // (2 * SUBLANES) - 1
    return pl.pallas_call(
        edge_kernel,
        grid=(members,),
        in_specs=[
            pl.BlockSpec(memory_space=pltpu.SMEM),
            pl.BlockSpec(factors.shape, lambda m: (0, 0)),
            pl.BlockSpec((1, fields, 2 * SUBLANES, width), lambda m: (m, 0, 0, 0)),
            pl.BlockSpec((1, fields, 2 * SUBLANES, width), lambda m: (m, 0, last, 0)),
            pl.BlockSpec((1, fields, margin, width), lambda m: (m, 0, 0, 0)),
            pl.BlockSpec((1, fields, margin, width), lambda m: (m, 0, 0, 0)),
        ],
        out_specs=[
            pl.BlockSpec((1, 2 * SUBLANES, width), lambda m: (m, 0, 0)),
            pl.BlockSpec((1, fields - 1, 2 * SUBLANES, width), lambda m: (m, 0, 0, 0)),
        ],
        out_shape=[
            jax.ShapeDtypeStruct((members, 2 * SUBLANES, width), jnp.float32),
            jax.ShapeDtypeStruct((members, fields - 1, 2 * SUBLANES, width), jnp.float32),
        ],
        scratch_shapes=[pltpu.VMEM((fields, 5 * SUBLANES, width), jnp.float32)] * 2,
        cost_estimate=forecast_cost(states, 6 * SUBLANES),
    )(inside, factors, states, states, before, after)


def tapering(cells, grid_width, block_cells, length):
    longitude = cells.astype(jnp.float32)
    tile_total = grid_width // block_cells
    centre = jnp.arange(tile_total).astype(jnp.float32) * block_cells + 0.5 * (block_cells - 1)
    distance = jnp.abs(longitude[..., :, None] - centre)
    distance = jnp.minimum(distance, grid_width - distance)
    return jnp.exp(-0.5 * (distance / length) ** 2)


def member_weights(heights, cells, values, block_cells, length):
    grid_width = heights.shape[-1]
    chosen_cells = (
        cells[:, None, :] == lax.broadcasted_iota(jnp.int32, (1, grid_width, 1), 1)
    ).astype(jnp.float32)
    observed = jnp.einsum("erl,rlo->reo", heights, chosen_cells, precision=lax.Precision.HIGHEST)
    misfit = (values[:, None, :] - observed) ** 2
    taper_weights = tapering(cells, grid_width, block_cells, length)
    likelihood = (
        -0.5
        / OBSERVATION_VARIANCE
        * jnp.einsum("reo,rob->rbe", misfit, taper_weights, precision=lax.Precision.HIGHEST)
    )
    largest = jnp.max(likelihood, axis=-1, keepdims=True)
    scaled = jnp.exp(likelihood - largest)
    return scaled / jnp.sum(scaled, axis=-1, keepdims=True)


def mixing_matrix(weights, draws):
    member_count = weights.shape[-1]
    split = draws.reshape(draws.shape[:-1] + (3, member_count))
    column = lax.broadcasted_iota(jnp.int32, (1, 1, 1, member_count), 3)
    picks = MERGE_FIRST * (split[:, :, 0, :, None] == column).astype(jnp.float32)
    picks = picks + BLEND_COEF_TWO * (split[:, :, 1, :, None] == column).astype(jnp.float32)
    picks = picks + MERGE_THIRD * (split[:, :, 2, :, None] == column).astype(jnp.float32)
    return (1.0 - RELAXATION) * weights[:, :, None, :] + RELAXATION * picks


def merge_fields(members, mixing, block_cells):
    member_count, fields, count_of_rows, grid_width = members.shape
    blocks = members.reshape(
        member_count, fields, count_of_rows, grid_width // block_cells, block_cells
    )
    updated = jnp.einsum("rbek,kfrbc->efrbc", mixing, blocks, precision=lax.Precision.HIGHEST)
    return updated.reshape(member_count, fields, count_of_rows, grid_width)


def shifts(count, d, targets):
    return [(i, (i + d) % count) for i in range(count) if (i + d) % count in targets]


def by_reach(count):
    return sorted(range(1, count), key=lambda d: abs(2 * d - count))


def send_all(pieces, axis, targets=None):
    count = lax.axis_size(axis)
    targets = range(count) if targets is None else targets
    received = {0: pieces[0]}
    for d in by_reach(count):
        received[d] = lax.ppermute(pieces[d], axis, shifts(count, d, targets))
    return [received[d] for d in range(count)]


def row_pieces(array, axis, dim):
    count = lax.axis_size(axis)
    own = lax.axis_index(axis)
    length = array.shape[dim] // count
    pieces = [
        lax.dynamic_slice_in_dim(array, lax.rem(own + d, count) * length, length, axis=dim)
        for d in range(count)
    ]
    return lax.optimization_barrier(pieces)


def edge_pieces(array, axis, dim, length):
    count = lax.axis_size(axis)
    own = lax.axis_index(axis)
    held = array.shape[dim]
    pieces = []
    for d in range(count):
        owner = lax.rem(own + d, count)
        start = jnp.where(2 * owner < count, owner * length, held - (count - owner) * length)
        pieces.append(lax.dynamic_slice_in_dim(array, start, length, axis=dim))
    return lax.optimization_barrier(pieces)


def put_back(whole, received, axis, field):
    count = lax.axis_size(axis)
    own = lax.axis_index(axis)
    length = received[0].shape[2]
    for d, piece in enumerate(received):
        start = lax.rem(own + count - d, count) * length
        whole = lax.dynamic_update_slice(whole, piece, (0, field, start, 0))
    return whole


def relative_draws(draws, axis, members_dev):
    count = lax.axis_size(axis)
    own = lax.axis_index(axis)
    distance = lax.rem(own + count - draws // members_dev, count)
    place = distance * members_dev + draws % members_dev
    split = place.reshape(place.shape[:-1] + (3, count, members_dev))
    doubled = jnp.concatenate([split, split], axis=-2)
    turned = lax.dynamic_slice_in_dim(doubled, own, count, axis=-2)
    return turned.reshape(draws.shape)


def body(particle_states, coriolis, observed_cells, observed_values, resample_draws):
    members_dev, _, count_of_rows, _ = particle_states.shape
    count = lax.axis_size("mem")
    own = lax.axis_index("mem")
    band_index = lax.axis_index("dom")
    margin = 2 * STEPS
    piece = count_of_rows // count
    inner = [
        j for j in range(count)
        if j * piece >= margin and (j + 1) * piece <= count_of_rows - margin
    ]
    outer = [j for j in range(count) if j not in inner]
    factors = coriolis_frame(coriolis, band_index, count_of_rows)

    before, after = edge_rows(particle_states, "dom", 2, margin)
    heights, winds = early_pieces(particle_states, factors, "mem")
    inner_heights = send_all(heights, "mem", inner)
    edges = edge_forecast(particle_states, before, after, factors, band_index, lax.axis_size("dom"))
    outer_heights = send_all(edge_pieces(edges[0], "mem", 1, piece), "mem", outer)
    inner_winds = send_all(winds, "mem", inner)
    outer_winds = send_all(edge_pieces(edges[1], "mem", 2, piece), "mem", outer)
    inner_heights, outer_heights = lax.optimization_barrier((inner_heights, outer_heights))
    is_outer = jnp.any(jnp.stack([own == j for j in outer]))

    def gather(at_edge, within):
        return jnp.concatenate(
            [jnp.where(is_outer, a, b) for a, b in zip(at_edge, within)], axis=0
        )

    heights = gather(outer_heights, inner_heights)
    winds_all = gather(outer_winds, inner_winds)

    cells = observed_cells[0]
    values = observed_values[0]
    draws = relative_draws(resample_draws[0], "mem", members_dev)
    weights = member_weights(heights, cells, values, LBLK, LOC)
    mixing = mixing_matrix(weights, draws)

    def hand_back(members):
        updated = merge_fields(members, mixing, LBLK)
        pieces = [updated[d * members_dev : (d + 1) * members_dev] for d in range(count)]
        return send_all(pieces, "mem")

    analysed = jnp.zeros(particle_states.shape, particle_states.dtype)
    analysed = put_back(analysed, hand_back(heights[:, None]), "mem", 0)
    return put_back(analysed, hand_back(winds_all), "mem", 1)


def solution(mesh):
    return jax.shard_map(
        body,
        mesh=mesh,
        in_specs=(
            P("mem", None, "dom", None),
            P(),
            P("dom", "mem", None),
            P("dom", "mem", None),
            P("dom", "mem", None, None),
        ),
        out_specs=P("mem", None, "dom", None),
        check_vma=False,
    )
```

```python
import functools

import jax
import jax.numpy as jnp
from jax import lax
from jax.experimental import pallas as pl
from jax.experimental.pallas import tpu as pltpu
from jax.sharding import PartitionSpec as P

LBLK = 128
LOC = 64
STEPS = 2
SUBLANES = 8
LANES = 128


FLOW_FACTOR = 1.0
PRESSURE_FACTOR = 1.0
OBSERVATION_VARIANCE = 16.0
RELAXATION = 0.5
MERGE_FIRST = 0.75
BLEND_COEF_TWO = (13.0**0.5 + 1.0) / 8.0
MERGE_THIRD = -(13.0**0.5 - 1.0) / 8.0


def edge_rows(array, axis, dim, width):
    count, length = (lax.axis_size(axis), array.shape[dim])
    up = [(i, i + 1) for i in range(count - 1)]
    down = [(j, i) for i, j in up]
    before = lax.ppermute(lax.slice_in_dim(array, length - width, length, axis=dim), axis, up)
    after = lax.ppermute(lax.slice_in_dim(array, 0, width, axis=dim), axis, down)
    return before, after


def forecast_steps(here, there, tiles, final, masked, factor):
    width = here.shape[2]

    def tile(t, shift=0):
        return slice(t * SUBLANES + shift, (t + 1) * SUBLANES + shift)

    def east(quantity):
        return pltpu.roll(quantity, width - 1, 1) - pltpu.roll(quantity, 1, 1)

    def north(ref, field, t):
        return ref[field, tile(t, 1), :] - ref[field, tile(t, -1), :]

    old, new = here, there
    for step in range(STEPS):
        for t in tiles:
            slope = east(old[1, tile(t), :]) + north(old, 2, t)
            new[0, tile(t), :] = masked(
                old[0, tile(t), :] - (0.5 * FLOW_FACTOR) * slope, t
            )
        for t in final if step == STEPS - 1 else tiles:
            turn = factor(t)
            east_old, north_old = old[1, tile(t), :], old[2, tile(t), :]
            east_new = (
                east_old - (0.5 * PRESSURE_FACTOR) * east(new[0, tile(t), :]) + turn * north_old
            )
            north_new = north_old - (0.5 * PRESSURE_FACTOR) * north(new, 0, t) - turn * east_old
            new[1, tile(t), :] = masked(east_new, t)
            new[2, tile(t), :] = masked(north_new, t)
        old, new = new, old
    return old


def coriolis_tile(coriolis_ref, t, width):
    factors = coriolis_ref[t * SUBLANES : (t + 1) * SUBLANES, :]
    return jnp.concatenate([factors] * (width // LANES), axis=1)


def forecast_kernel(count, place_ref, inside_ref, coriolis_ref, states_ref, before_ref, after_ref, *refs):
    rows, width = states_ref.shape[2:]
    margin = before_ref.shape[2]
    outs, (here, there) = refs[:-2], refs[-2:]
    first = 2 * SUBLANES
    last = rows // SUBLANES + 2
    here[:, first - margin : first, :] = before_ref[0]
    here[:, first : first + rows, :] = states_ref[0]
    here[:, first + rows : first + rows + margin, :] = after_ref[0]

    def masked(quantity, t):
        if t == 1:
            return quantity * inside_ref[0]
        if t == last:
            return quantity * inside_ref[1]
        return quantity

    done = forecast_steps(
        here, there, range(1, last + 1), range(2, last), masked,
        lambda t: coriolis_tile(coriolis_ref, t, width),
    )
    if len(outs) == 2:
        outs[0][0] = done[0, first : first + rows, :]
        outs[1][0] = done[1:, first : first + rows, :]
        return
    piece = rows // count
    for d in range(count):
        start = pl.multiple_of(lax.rem(place_ref[0] + d, count) * piece, SUBLANES)
        outs[d][0] = done[0, pl.ds(first + start, piece), :]
        outs[count + d][0] = done[1:, pl.ds(first + start, piece), :]


def coriolis_frame(coriolis, band_index, rows):
    padded = jnp.pad(coriolis, (2 * SUBLANES, 2 * SUBLANES))
    spread = jnp.broadcast_to(padded[:, None], padded.shape + (LANES,))
    return lax.dynamic_slice_in_dim(spread, band_index * rows, rows + 4 * SUBLANES)


def forecast_cost(states, rows):
    size = states.size * rows // states.shape[2]
    return pl.CostEstimate(flops=40 * size * STEPS, bytes_accessed=8 * size, transcendentals=0)


def forecast_pieces(states, before, after, factors, axis, band_index, band_count):
    members, fields, rows, width = states.shape
    count = lax.axis_size(axis)
    margin = before.shape[2]
    piece = rows // count
    whole = piece % SUBLANES != 0
    extents = (rows,) if whole else (piece,) * count
    place = lax.axis_index(axis).astype(jnp.int32).reshape(1)
    inside = jnp.stack([band_index > 0, band_index < band_count - 1]).astype(jnp.float32)
    found = pl.pallas_call(
        functools.partial(forecast_kernel, count),
        grid=(members,),
        in_specs=[
            pl.BlockSpec(memory_space=pltpu.SMEM),
            pl.BlockSpec(memory_space=pltpu.SMEM),
            pl.BlockSpec(factors.shape, lambda m: (0, 0)),
            pl.BlockSpec((1, fields, rows, width), lambda m: (m, 0, 0, 0)),
            pl.BlockSpec((1, fields, margin, width), lambda m: (m, 0, 0, 0)),
            pl.BlockSpec((1, fields, margin, width), lambda m: (m, 0, 0, 0)),
        ],
        out_specs=[pl.BlockSpec((1, r, width), lambda m: (m, 0, 0)) for r in extents]
        + [pl.BlockSpec((1, fields - 1, r, width), lambda m: (m, 0, 0, 0)) for r in extents],
        out_shape=[jax.ShapeDtypeStruct((members, r, width), jnp.float32) for r in extents]
        + [jax.ShapeDtypeStruct((members, fields - 1, r, width), jnp.float32) for r in extents],
        scratch_shapes=[pltpu.VMEM((fields, factors.shape[0], width), jnp.float32)] * 2,
        cost_estimate=forecast_cost(states, rows),
    )(place, inside, factors, states, before, after)
    if whole:
        return row_pieces(found[0], axis, 1), row_pieces(found[1], axis, 2)
    return list(found[:count]), list(found[count:])


def tapering(cells, grid_width, block_cells, length):
    longitude = cells.astype(jnp.float32)
    tile_total = grid_width // block_cells
    centre = jnp.arange(tile_total).astype(jnp.float32) * block_cells + 0.5 * (block_cells - 1)
    distance = jnp.abs(longitude[..., :, None] - centre)
    distance = jnp.minimum(distance, grid_width - distance)
    return jnp.exp(-0.5 * (distance / length) ** 2)


def member_weights(heights, cells, values, block_cells, length):
    grid_width = heights.shape[-1]
    chosen_cells = (
        cells[:, None, :] == lax.broadcasted_iota(jnp.int32, (1, grid_width, 1), 1)
    ).astype(jnp.float32)
    observed = jnp.einsum("erl,rlo->reo", heights, chosen_cells, precision=lax.Precision.HIGHEST)
    misfit = (values[:, None, :] - observed) ** 2
    taper_weights = tapering(cells, grid_width, block_cells, length)
    likelihood = (
        -0.5
        / OBSERVATION_VARIANCE
        * jnp.einsum("reo,rob->rbe", misfit, taper_weights, precision=lax.Precision.HIGHEST)
    )
    largest = jnp.max(likelihood, axis=-1, keepdims=True)
    scaled = jnp.exp(likelihood - largest)
    return scaled / jnp.sum(scaled, axis=-1, keepdims=True)


def mixing_matrix(weights, draws):
    member_count = weights.shape[-1]
    split = draws.reshape(draws.shape[:-1] + (3, member_count))
    column = lax.broadcasted_iota(jnp.int32, (1, 1, 1, member_count), 3)
    picks = MERGE_FIRST * (split[:, :, 0, :, None] == column).astype(jnp.float32)
    picks = picks + BLEND_COEF_TWO * (split[:, :, 1, :, None] == column).astype(jnp.float32)
    picks = picks + MERGE_THIRD * (split[:, :, 2, :, None] == column).astype(jnp.float32)
    return (1.0 - RELAXATION) * weights[:, :, None, :] + RELAXATION * picks


def merge_fields(members, mixing, block_cells):
    member_count, fields, count_of_rows, grid_width = members.shape
    blocks = members.reshape(
        member_count, fields, count_of_rows, grid_width // block_cells, block_cells
    )
    updated = jnp.einsum("rbek,kfrbc->efrbc", mixing, blocks, precision=lax.Precision.HIGHEST)
    return updated.reshape(member_count, fields, count_of_rows, grid_width)


def send_all(pieces, axis):
    count = lax.axis_size(axis)
    received = [pieces[0]]
    for d in range(1, count):
        received.append(lax.ppermute(pieces[d], axis, [(i, (i + d) % count) for i in range(count)]))
    return received


def row_pieces(array, axis, dim):
    count = lax.axis_size(axis)
    own = lax.axis_index(axis)
    length = array.shape[dim] // count
    return [
        lax.dynamic_slice_in_dim(array, lax.rem(own + d, count) * length, length, axis=dim)
        for d in range(count)
    ]


def put_back(whole, received, axis, field):
    count = lax.axis_size(axis)
    own = lax.axis_index(axis)
    length = received[0].shape[2]
    for d, piece in enumerate(received):
        start = lax.rem(own + count - d, count) * length
        whole = lax.dynamic_update_slice(whole, piece, (0, field, start, 0))
    return whole


def relative_draws(draws, axis, members_dev):
    count = lax.axis_size(axis)
    own = lax.axis_index(axis)
    distance = lax.rem(own + count - draws // members_dev, count)
    place = distance * members_dev + draws % members_dev
    split = place.reshape(place.shape[:-1] + (3, count, members_dev))
    doubled = jnp.concatenate([split, split], axis=-2)
    turned = lax.dynamic_slice_in_dim(doubled, own, count, axis=-2)
    return turned.reshape(draws.shape)


def body(particle_states, coriolis, observed_cells, observed_values, resample_draws):
    members_dev, fields, count_of_rows, grid_width = particle_states.shape
    count = lax.axis_size("mem")
    band_index = lax.axis_index("dom")
    factors = coriolis_frame(coriolis, band_index, count_of_rows)
    before, after = edge_rows(particle_states, "dom", 2, 2 * STEPS)
    heights, winds = forecast_pieces(
        particle_states, before, after, factors, "mem", band_index, lax.axis_size("dom")
    )
    heights = jnp.concatenate(send_all(heights, "mem"), axis=0)
    winds_all = jnp.concatenate(send_all(winds, "mem"), axis=0)

    cells = observed_cells[0]
    values = observed_values[0]
    draws = relative_draws(resample_draws[0], "mem", members_dev)
    weights = member_weights(heights, cells, values, LBLK, LOC)
    mixing = mixing_matrix(weights, draws)

    def hand_back(members):
        updated = merge_fields(members, mixing, LBLK)
        pieces = [updated[d * members_dev : (d + 1) * members_dev] for d in range(count)]
        return send_all(pieces, "mem")

    analysed = jnp.zeros(particle_states.shape, particle_states.dtype)
    analysed = put_back(analysed, hand_back(heights[:, None]), "mem", 0)
    return put_back(analysed, hand_back(winds_all), "mem", 1)


def solution(mesh):
    return jax.shard_map(
        body,
        mesh=mesh,
        in_specs=(
            P("mem", None, "dom", None),
            P(),
            P("dom", "mem", None),
            P("dom", "mem", None),
            P("dom", "mem", None, None),
        ),
        out_specs=P("mem", None, "dom", None),
        check_vma=False,
    )
```

```python
import functools

import jax
import jax.numpy as jnp
from jax import lax
from jax.experimental import pallas as pl
from jax.experimental.pallas import tpu as pltpu
from jax.sharding import PartitionSpec as P


LBLK = 128
LOC = 64
STEPS = 2
SUBLANES = 8
LANES = 128


FLOW_FACTOR = 1.0
PRESSURE_FACTOR = 1.0
OBSERVATION_VARIANCE = 16.0
RELAXATION = 0.5
MERGE_FIRST = 0.75
BLEND_COEF_TWO = (13.0**0.5 + 1.0) / 8.0
MERGE_THIRD = -(13.0**0.5 - 1.0) / 8.0


def edge_rows(array, axis, dim, width):
    count, length = (lax.axis_size(axis), array.shape[dim])
    up = [(i, i + 1) for i in range(count - 1)]
    down = [(j, i) for i, j in up]
    before = lax.ppermute(lax.slice_in_dim(array, length - width, length, axis=dim), axis, up)
    after = lax.ppermute(lax.slice_in_dim(array, 0, width, axis=dim), axis, down)
    return before, after


def forecast_steps(here, there, tiles, final, masked, factor):
    width = here.shape[2]

    def tile(t, shift=0):
        return slice(t * SUBLANES + shift, (t + 1) * SUBLANES + shift)

    def east(quantity):
        return pltpu.roll(quantity, width - 1, 1) - pltpu.roll(quantity, 1, 1)

    def north(ref, field, t):
        return ref[field, tile(t, 1), :] - ref[field, tile(t, -1), :]

    old, new = here, there
    for step in range(STEPS):
        for t in tiles:
            slope = east(old[1, tile(t), :]) + north(old, 2, t)
            new[0, tile(t), :] = masked(
                old[0, tile(t), :] - (0.5 * FLOW_FACTOR) * slope, t
            )
        for t in final if step == STEPS - 1 else tiles:
            turn = factor(t)
            east_old, north_old = old[1, tile(t), :], old[2, tile(t), :]
            east_new = (
                east_old - (0.5 * PRESSURE_FACTOR) * east(new[0, tile(t), :]) + turn * north_old
            )
            north_new = north_old - (0.5 * PRESSURE_FACTOR) * north(new, 0, t) - turn * east_old
            new[1, tile(t), :] = masked(east_new, t)
            new[2, tile(t), :] = masked(north_new, t)
        old, new = new, old
    return old


def coriolis_tile(coriolis_ref, t, width):
    factors = coriolis_ref[t * SUBLANES : (t + 1) * SUBLANES, :]
    return jnp.concatenate([factors] * (width // LANES), axis=1)


def forecast_kernel(count, place_ref, inside_ref, coriolis_ref, states_ref, before_ref, after_ref, *refs):
    rows, width = states_ref.shape[2:]
    margin = before_ref.shape[2]
    outs, (here, there) = refs[:-2], refs[-2:]
    first = 2 * SUBLANES
    last = rows // SUBLANES + 2
    here[:, first - margin : first, :] = before_ref[0]
    here[:, first : first + rows, :] = states_ref[0]
    here[:, first + rows : first + rows + margin, :] = after_ref[0]

    def masked(quantity, t):
        if t == 1:
            return quantity * inside_ref[0]
        if t == last:
            return quantity * inside_ref[1]
        return quantity

    done = forecast_steps(
        here, there, range(1, last + 1), range(2, last), masked,
        lambda t: coriolis_tile(coriolis_ref, t, width),
    )
    if len(outs) == 2:
        outs[0][0] = done[0, first : first + rows, :]
        outs[1][0] = done[1:, first : first + rows, :]
        return
    piece = rows // count
    for d in range(count):
        start = pl.multiple_of(lax.rem(place_ref[0] + d, count) * piece, SUBLANES)
        outs[d][0] = done[0, pl.ds(first + start, piece), :]
        outs[count + d][0] = done[1:, pl.ds(first + start, piece), :]


def coriolis_frame(coriolis, band_index, rows):
    padded = jnp.pad(coriolis, (2 * SUBLANES, 2 * SUBLANES))
    spread = jnp.broadcast_to(padded[:, None], padded.shape + (LANES,))
    return lax.dynamic_slice_in_dim(spread, band_index * rows, rows + 4 * SUBLANES)


def forecast_cost(states, rows):
    size = states.size * rows // states.shape[2]
    return pl.CostEstimate(flops=40 * size * STEPS, bytes_accessed=8 * size, transcendentals=0)


def forecast_pieces(states, before, after, factors, axis, band_index, band_count):
    members, fields, rows, width = states.shape
    count = lax.axis_size(axis)
    margin = before.shape[2]
    piece = rows // count
    whole = piece % SUBLANES != 0
    extents = (rows,) if whole else (piece,) * count
    place = lax.axis_index(axis).astype(jnp.int32).reshape(1)
    inside = jnp.stack([band_index > 0, band_index < band_count - 1]).astype(jnp.float32)
    found = pl.pallas_call(
        functools.partial(forecast_kernel, count),
        grid=(members,),
        in_specs=[
            pl.BlockSpec(memory_space=pltpu.SMEM),
            pl.BlockSpec(memory_space=pltpu.SMEM),
            pl.BlockSpec(factors.shape, lambda m: (0, 0)),
            pl.BlockSpec((1, fields, rows, width), lambda m: (m, 0, 0, 0)),
            pl.BlockSpec((1, fields, margin, width), lambda m: (m, 0, 0, 0)),
            pl.BlockSpec((1, fields, margin, width), lambda m: (m, 0, 0, 0)),
        ],
        out_specs=[pl.BlockSpec((1, r, width), lambda m: (m, 0, 0)) for r in extents]
        + [pl.BlockSpec((1, fields - 1, r, width), lambda m: (m, 0, 0, 0)) for r in extents],
        out_shape=[jax.ShapeDtypeStruct((members, r, width), jnp.float32) for r in extents]
        + [jax.ShapeDtypeStruct((members, fields - 1, r, width), jnp.float32) for r in extents],
        scratch_shapes=[pltpu.VMEM((fields, factors.shape[0], width), jnp.float32)] * 2,
        cost_estimate=forecast_cost(states, rows),
    )(place, inside, factors, states, before, after)
    if whole:
        return row_pieces(found[0], axis, 1), row_pieces(found[1], axis, 2)
    return list(found[:count]), list(found[count:])


def tapering(cells, grid_width, block_cells, length):
    longitude = cells.astype(jnp.float32)
    tile_total = grid_width // block_cells
    centre = jnp.arange(tile_total).astype(jnp.float32) * block_cells + 0.5 * (block_cells - 1)
    distance = jnp.abs(longitude[..., :, None] - centre)
    distance = jnp.minimum(distance, grid_width - distance)
    return jnp.exp(-0.5 * (distance / length) ** 2)


def member_weights(heights, cells, values, block_cells, length):
    grid_width = heights.shape[-1]
    chosen_cells = (
        cells[:, None, :] == lax.broadcasted_iota(jnp.int32, (1, grid_width, 1), 1)
    ).astype(jnp.float32)
    observed = jnp.einsum("erl,rlo->reo", heights, chosen_cells, precision=lax.Precision.HIGHEST)
    misfit = (values[:, None, :] - observed) ** 2
    taper_weights = tapering(cells, grid_width, block_cells, length)
    likelihood = (
        -0.5
        / OBSERVATION_VARIANCE
        * jnp.einsum("reo,rob->rbe", misfit, taper_weights, precision=lax.Precision.HIGHEST)
    )
    largest = jnp.max(likelihood, axis=-1, keepdims=True)
    scaled = jnp.exp(likelihood - largest)
    return scaled / jnp.sum(scaled, axis=-1, keepdims=True)


def mixing_matrix(weights, draws):
    member_count = weights.shape[-1]
    split = draws.reshape(draws.shape[:-1] + (3, member_count))
    column = lax.broadcasted_iota(jnp.int32, (1, 1, 1, member_count), 3)
    picks = MERGE_FIRST * (split[:, :, 0, :, None] == column).astype(jnp.float32)
    picks = picks + BLEND_COEF_TWO * (split[:, :, 1, :, None] == column).astype(jnp.float32)
    picks = picks + MERGE_THIRD * (split[:, :, 2, :, None] == column).astype(jnp.float32)
    return (1.0 - RELAXATION) * weights[:, :, None, :] + RELAXATION * picks


def merge_fields(members, mixing, block_cells):
    member_count, fields, count_of_rows, grid_width = members.shape
    blocks = members.reshape(
        member_count, fields, count_of_rows, grid_width // block_cells, block_cells
    )
    updated = jnp.einsum("rbek,kfrbc->efrbc", mixing, blocks, precision=lax.Precision.HIGHEST)
    return updated.reshape(member_count, fields, count_of_rows, grid_width)


def send_all(pieces, axis):
    count = lax.axis_size(axis)
    received = [pieces[0]]
    for d in range(1, count):
        received.append(lax.ppermute(pieces[d], axis, [(i, (i + d) % count) for i in range(count)]))
    return received


def row_pieces(array, axis, dim):
    count = lax.axis_size(axis)
    own = lax.axis_index(axis)
    length = array.shape[dim] // count
    return [
        lax.dynamic_slice_in_dim(array, lax.rem(own + d, count) * length, length, axis=dim)
        for d in range(count)
    ]


def put_back(whole, received, axis, field):
    count = lax.axis_size(axis)
    own = lax.axis_index(axis)
    length = received[0].shape[2]
    for d, piece in enumerate(received):
        start = lax.rem(own + count - d, count) * length
        whole = lax.dynamic_update_slice(whole, piece, (0, field, start, 0))
    return whole


def relative_draws(draws, axis, members_dev):
    count = lax.axis_size(axis)
    own = lax.axis_index(axis)
    distance = lax.rem(own + count - draws // members_dev, count)
    place = distance * members_dev + draws % members_dev
    split = place.reshape(place.shape[:-1] + (3, count, members_dev))
    doubled = jnp.concatenate([split, split], axis=-2)
    turned = lax.dynamic_slice_in_dim(doubled, own, count, axis=-2)
    return turned.reshape(draws.shape)


def body(particle_states, coriolis, observed_cells, observed_values, resample_draws):
    members_dev, _, count_of_rows, _ = particle_states.shape
    count = lax.axis_size("mem")
    band_index = lax.axis_index("dom")
    factors = coriolis_frame(coriolis, band_index, count_of_rows)
    before, after = edge_rows(particle_states, "dom", 2, 2 * STEPS)
    heights, winds = forecast_pieces(
        particle_states, before, after, factors, "mem", band_index, lax.axis_size("dom")
    )
    heights = send_all(heights, "mem")
    winds_all = send_all(winds, "mem")
    heights = jnp.concatenate(heights, axis=0)
    winds_all = jnp.concatenate(winds_all, axis=0)

    cells = observed_cells[0]
    values = observed_values[0]
    draws = relative_draws(resample_draws[0], "mem", members_dev)
    weights = member_weights(heights, cells, values, LBLK, LOC)
    mixing = mixing_matrix(weights, draws)

    def hand_back(members):
        updated = merge_fields(members, mixing, LBLK)
        pieces = [updated[d * members_dev : (d + 1) * members_dev] for d in range(count)]
        return send_all(pieces, "mem")

    analysed = jnp.zeros(particle_states.shape, particle_states.dtype)
    analysed = put_back(analysed, hand_back(heights[:, None]), "mem", 0)
    return put_back(analysed, hand_back(winds_all), "mem", 1)


def solution(mesh):
    return jax.shard_map(
        body,
        mesh=mesh,
        in_specs=(
            P("mem", None, "dom", None),
            P(),
            P("dom", "mem", None),
            P("dom", "mem", None),
            P("dom", "mem", None, None),
        ),
        out_specs=P("mem", None, "dom", None),
        check_vma=False,
    )
```

```python
import functools

import jax
import jax.numpy as jnp
from jax import lax
from jax.experimental import pallas as pl
from jax.experimental.pallas import tpu as pltpu
from jax.sharding import PartitionSpec as P


LBLK = 128
LOC = 64
STEPS = 2
SUBLANES = 8
LANES = 128


FLOW_FACTOR = 1.0
PRESSURE_FACTOR = 1.0
OBSERVATION_VARIANCE = 16.0
RELAXATION = 0.5
MERGE_FIRST = 0.75
BLEND_COEF_TWO = (13.0**0.5 + 1.0) / 8.0
MERGE_THIRD = -(13.0**0.5 - 1.0) / 8.0


def edge_rows(array, axis, dim, width):
    count, length = (lax.axis_size(axis), array.shape[dim])
    up = [(i, i + 1) for i in range(count - 1)]
    down = [(j, i) for i, j in up]
    before = lax.ppermute(lax.slice_in_dim(array, length - width, length, axis=dim), axis, up)
    after = lax.ppermute(lax.slice_in_dim(array, 0, width, axis=dim), axis, down)
    return before, after


def forecast_steps(here, there, tiles, final, masked, factor):
    width = here.shape[2]

    def tile(t, shift=0):
        return slice(t * SUBLANES + shift, (t + 1) * SUBLANES + shift)

    def east(quantity):
        return pltpu.roll(quantity, width - 1, 1) - pltpu.roll(quantity, 1, 1)

    def north(ref, field, t):
        return ref[field, tile(t, 1), :] - ref[field, tile(t, -1), :]

    old, new = here, there
    for step in range(STEPS):
        for t in tiles:
            slope = east(old[1, tile(t), :]) + north(old, 2, t)
            new[0, tile(t), :] = masked(
                old[0, tile(t), :] - (0.5 * FLOW_FACTOR) * slope, t
            )
        for t in final if step == STEPS - 1 else tiles:
            turn = factor(t)
            east_old, north_old = old[1, tile(t), :], old[2, tile(t), :]
            east_new = (
                east_old - (0.5 * PRESSURE_FACTOR) * east(new[0, tile(t), :]) + turn * north_old
            )
            north_new = north_old - (0.5 * PRESSURE_FACTOR) * north(new, 0, t) - turn * east_old
            new[1, tile(t), :] = masked(east_new, t)
            new[2, tile(t), :] = masked(north_new, t)
        old, new = new, old
    return old


def coriolis_tile(coriolis_ref, t, width):
    factors = coriolis_ref[t * SUBLANES : (t + 1) * SUBLANES, :]
    return jnp.concatenate([factors] * (width // LANES), axis=1)


def forecast_kernel(count, place_ref, inside_ref, coriolis_ref, states_ref, before_ref, after_ref, *refs):
    rows, width = states_ref.shape[2:]
    margin = before_ref.shape[2]
    outs, (here, there) = refs[:-2], refs[-2:]
    first = 2 * SUBLANES
    last = rows // SUBLANES + 2
    here[:, first - margin : first, :] = before_ref[0]
    here[:, first : first + rows, :] = states_ref[0]
    here[:, first + rows : first + rows + margin, :] = after_ref[0]

    def masked(quantity, t):
        if t == 1:
            return quantity * inside_ref[0]
        if t == last:
            return quantity * inside_ref[1]
        return quantity

    done = forecast_steps(
        here, there, range(1, last + 1), range(2, last), masked,
        lambda t: coriolis_tile(coriolis_ref, t, width),
    )
    if len(outs) == 2:
        outs[0][0] = done[0, first : first + rows, :]
        outs[1][0] = done[1:, first : first + rows, :]
        return
    piece = rows // count
    for d in range(count):
        start = pl.multiple_of(lax.rem(place_ref[0] + d, count) * piece, SUBLANES)
        outs[d][0] = done[0, pl.ds(first + start, piece), :]
        outs[count + d][0] = done[1:, pl.ds(first + start, piece), :]


def coriolis_frame(coriolis, band_index, rows):
    padded = jnp.pad(coriolis, (2 * SUBLANES, 2 * SUBLANES))
    spread = jnp.broadcast_to(padded[:, None], padded.shape + (LANES,))
    return lax.dynamic_slice_in_dim(spread, band_index * rows, rows + 4 * SUBLANES)


def forecast_cost(states, rows):
    size = states.size * rows // states.shape[2]
    return pl.CostEstimate(flops=40 * size * STEPS, bytes_accessed=8 * size, transcendentals=0)


def forecast_pieces(states, before, after, factors, axis, band_index, band_count):
    members, fields, rows, width = states.shape
    count = lax.axis_size(axis)
    margin = before.shape[2]
    piece = rows // count
    whole = piece % SUBLANES != 0
    extents = (rows,) if whole else (piece,) * count
    place = lax.axis_index(axis).astype(jnp.int32).reshape(1)
    inside = jnp.stack([band_index > 0, band_index < band_count - 1]).astype(jnp.float32)
    found = pl.pallas_call(
        functools.partial(forecast_kernel, count),
        grid=(members,),
        in_specs=[
            pl.BlockSpec(memory_space=pltpu.SMEM),
            pl.BlockSpec(memory_space=pltpu.SMEM),
            pl.BlockSpec(factors.shape, lambda m: (0, 0)),
            pl.BlockSpec((1, fields, rows, width), lambda m: (m, 0, 0, 0)),
            pl.BlockSpec((1, fields, margin, width), lambda m: (m, 0, 0, 0)),
            pl.BlockSpec((1, fields, margin, width), lambda m: (m, 0, 0, 0)),
        ],
        out_specs=[pl.BlockSpec((1, r, width), lambda m: (m, 0, 0)) for r in extents]
        + [pl.BlockSpec((1, fields - 1, r, width), lambda m: (m, 0, 0, 0)) for r in extents],
        out_shape=[jax.ShapeDtypeStruct((members, r, width), jnp.float32) for r in extents]
        + [jax.ShapeDtypeStruct((members, fields - 1, r, width), jnp.float32) for r in extents],
        scratch_shapes=[pltpu.VMEM((fields, factors.shape[0], width), jnp.float32)] * 2,
        cost_estimate=forecast_cost(states, rows),
    )(place, inside, factors, states, before, after)
    if whole:
        return row_pieces(found[0], axis, 1), row_pieces(found[1], axis, 2)
    return list(found[:count]), list(found[count:])


def tapering(cells, grid_width, block_cells, length):
    longitude = cells.astype(jnp.float32)
    tile_total = grid_width // block_cells
    centre = jnp.arange(tile_total).astype(jnp.float32) * block_cells + 0.5 * (block_cells - 1)
    distance = jnp.abs(longitude[..., :, None] - centre)
    distance = jnp.minimum(distance, grid_width - distance)
    return jnp.exp(-0.5 * (distance / length) ** 2)


def member_weights(heights, cells, values, block_cells, length):
    grid_width = heights.shape[-1]
    chosen_cells = (
        cells[:, None, :] == lax.broadcasted_iota(jnp.int32, (1, grid_width, 1), 1)
    ).astype(jnp.float32)
    observed = jnp.einsum("erl,rlo->reo", heights, chosen_cells, precision=lax.Precision.HIGHEST)
    misfit = (values[:, None, :] - observed) ** 2
    taper_weights = tapering(cells, grid_width, block_cells, length)
    likelihood = (
        -0.5
        / OBSERVATION_VARIANCE
        * jnp.einsum("reo,rob->rbe", misfit, taper_weights, precision=lax.Precision.HIGHEST)
    )
    largest = jnp.max(likelihood, axis=-1, keepdims=True)
    scaled = jnp.exp(likelihood - largest)
    return scaled / jnp.sum(scaled, axis=-1, keepdims=True)


def mixing_matrix(weights, draws):
    member_count = weights.shape[-1]
    split = draws.reshape(draws.shape[:-1] + (3, member_count))
    column = lax.broadcasted_iota(jnp.int32, (1, 1, 1, member_count), 3)
    picks = MERGE_FIRST * (split[:, :, 0, :, None] == column).astype(jnp.float32)
    picks = picks + BLEND_COEF_TWO * (split[:, :, 1, :, None] == column).astype(jnp.float32)
    picks = picks + MERGE_THIRD * (split[:, :, 2, :, None] == column).astype(jnp.float32)
    return (1.0 - RELAXATION) * weights[:, :, None, :] + RELAXATION * picks


def merge_fields(members, mixing, block_cells):
    member_count, fields, count_of_rows, grid_width = members.shape
    blocks = members.reshape(
        member_count, fields, count_of_rows, grid_width // block_cells, block_cells
    )
    updated = jnp.einsum("rbek,kfrbc->efrbc", mixing, blocks, precision=lax.Precision.HIGHEST)
    return updated.reshape(member_count, fields, count_of_rows, grid_width)


def by_reach(count):
    return sorted(range(1, count), key=lambda d: abs(2 * d - count))


def send_all(pieces, axis):
    count = lax.axis_size(axis)
    received = {0: pieces[0]}
    for d in by_reach(count):
        received[d] = lax.ppermute(pieces[d], axis, [(i, (i + d) % count) for i in range(count)])
    return [received[d] for d in range(count)]


def row_pieces(array, axis, dim):
    count = lax.axis_size(axis)
    own = lax.axis_index(axis)
    length = array.shape[dim] // count
    return [
        lax.dynamic_slice_in_dim(array, lax.rem(own + d, count) * length, length, axis=dim)
        for d in range(count)
    ]


def put_back(whole, received, axis, field):
    count = lax.axis_size(axis)
    own = lax.axis_index(axis)
    length = received[0].shape[2]
    for d in [0] + by_reach(count)[::-1]:
        piece = received[d]
        start = lax.rem(own + count - d, count) * length
        whole = lax.dynamic_update_slice(whole, piece, (0, field, start, 0))
    return whole


def relative_draws(draws, axis, members_dev):
    count = lax.axis_size(axis)
    own = lax.axis_index(axis)
    distance = lax.rem(own + count - draws // members_dev, count)
    place = distance * members_dev + draws % members_dev
    split = place.reshape(place.shape[:-1] + (3, count, members_dev))
    doubled = jnp.concatenate([split, split], axis=-2)
    turned = lax.dynamic_slice_in_dim(doubled, own, count, axis=-2)
    return turned.reshape(draws.shape)


def body(particle_states, coriolis, observed_cells, observed_values, resample_draws):
    members_dev, _, count_of_rows, _ = particle_states.shape
    count = lax.axis_size("mem")
    band_index = lax.axis_index("dom")
    factors = coriolis_frame(coriolis, band_index, count_of_rows)
    before, after = edge_rows(particle_states, "dom", 2, 2 * STEPS)
    heights, winds = forecast_pieces(
        particle_states, before, after, factors, "mem", band_index, lax.axis_size("dom")
    )
    heights = send_all(heights, "mem")
    winds_all = send_all(winds, "mem")
    heights = jnp.concatenate(heights, axis=0)
    winds_all = jnp.concatenate(winds_all, axis=0)

    cells = observed_cells[0]
    values = observed_values[0]
    draws = relative_draws(resample_draws[0], "mem", members_dev)
    weights = member_weights(heights, cells, values, LBLK, LOC)
    mixing = mixing_matrix(weights, draws)

    def hand_back(members):
        updated = merge_fields(members, mixing, LBLK)
        pieces = [updated[d * members_dev : (d + 1) * members_dev] for d in range(count)]
        return send_all(pieces, "mem")

    analysed = jnp.zeros(particle_states.shape, particle_states.dtype)
    analysed = put_back(analysed, hand_back(heights[:, None]), "mem", 0)
    return put_back(analysed, hand_back(winds_all), "mem", 1)


def solution(mesh):
    return jax.shard_map(
        body,
        mesh=mesh,
        in_specs=(
            P("mem", None, "dom", None),
            P(),
            P("dom", "mem", None),
            P("dom", "mem", None),
            P("dom", "mem", None, None),
        ),
        out_specs=P("mem", None, "dom", None),
        check_vma=False,
    )
```

```python
import functools

import jax
import jax.numpy as jnp
from jax import lax
from jax.experimental import pallas as pl
from jax.experimental.pallas import tpu as pltpu
from jax.sharding import PartitionSpec as P


LBLK = 128
LOC = 64
STEPS = 2
SUBLANES = 8
LANES = 128


FLOW_FACTOR = 1.0
PRESSURE_FACTOR = 1.0
OBSERVATION_VARIANCE = 16.0
RELAXATION = 0.5
MERGE_FIRST = 0.75
BLEND_COEF_TWO = (13.0**0.5 + 1.0) / 8.0
MERGE_THIRD = -(13.0**0.5 - 1.0) / 8.0


def edge_rows(array, axis, dim, width):
    count, length = (lax.axis_size(axis), array.shape[dim])
    up = [(i, i + 1) for i in range(count - 1)]
    down = [(j, i) for i, j in up]
    before = lax.ppermute(lax.slice_in_dim(array, length - width, length, axis=dim), axis, up)
    after = lax.ppermute(lax.slice_in_dim(array, 0, width, axis=dim), axis, down)
    return before, after


def forecast_steps(here, there, tiles, final, masked, factor):
    width = here.shape[2]

    def tile(t, shift=0):
        return slice(t * SUBLANES + shift, (t + 1) * SUBLANES + shift)

    def east(quantity):
        return pltpu.roll(quantity, width - 1, 1) - pltpu.roll(quantity, 1, 1)

    def north(ref, field, t):
        return ref[field, tile(t, 1), :] - ref[field, tile(t, -1), :]

    old, new = here, there
    for step in range(STEPS):
        for t in tiles:
            slope = east(old[1, tile(t), :]) + north(old, 2, t)
            new[0, tile(t), :] = masked(
                old[0, tile(t), :] - (0.5 * FLOW_FACTOR) * slope, t
            )
        for t in final if step == STEPS - 1 else tiles:
            turn = factor(t)
            east_old, north_old = old[1, tile(t), :], old[2, tile(t), :]
            east_new = (
                east_old - (0.5 * PRESSURE_FACTOR) * east(new[0, tile(t), :]) + turn * north_old
            )
            north_new = north_old - (0.5 * PRESSURE_FACTOR) * north(new, 0, t) - turn * east_old
            new[1, tile(t), :] = masked(east_new, t)
            new[2, tile(t), :] = masked(north_new, t)
        old, new = new, old
    return old


def coriolis_tile(coriolis_ref, t, width):
    factors = coriolis_ref[t * SUBLANES : (t + 1) * SUBLANES, :]
    return jnp.concatenate([factors] * (width // LANES), axis=1)


def forecast_kernel(count, place_ref, inside_ref, coriolis_ref, states_ref, before_ref, after_ref, *refs):
    rows, width = states_ref.shape[2:]
    margin = before_ref.shape[2]
    outs, (here, there) = refs[:-2], refs[-2:]
    first = 2 * SUBLANES
    last = rows // SUBLANES + 2
    here[:, first - margin : first, :] = before_ref[0]
    here[:, first : first + rows, :] = states_ref[0]
    here[:, first + rows : first + rows + margin, :] = after_ref[0]

    def masked(quantity, t):
        if t == 1:
            return quantity * inside_ref[0]
        if t == last:
            return quantity * inside_ref[1]
        return quantity

    done = forecast_steps(
        here, there, range(1, last + 1), range(2, last), masked,
        lambda t: coriolis_tile(coriolis_ref, t, width),
    )
    if len(outs) == 2:
        outs[0][0] = done[0, first : first + rows, :]
        outs[1][0] = done[1:, first : first + rows, :]
        return
    piece = rows // count
    for d in range(count):
        start = pl.multiple_of(lax.rem(place_ref[0] + d, count) * piece, SUBLANES)
        outs[d][0] = done[0, pl.ds(first + start, piece), :]
        outs[count + d][0] = done[1:, pl.ds(first + start, piece), :]


def coriolis_frame(coriolis, band_index, rows):
    padded = jnp.pad(coriolis, (2 * SUBLANES, 2 * SUBLANES))
    spread = jnp.broadcast_to(padded[:, None], padded.shape + (LANES,))
    return lax.dynamic_slice_in_dim(spread, band_index * rows, rows + 4 * SUBLANES)


def forecast_cost(states, rows):
    size = states.size * rows // states.shape[2]
    return pl.CostEstimate(flops=40 * size * STEPS, bytes_accessed=8 * size, transcendentals=0)


def forecast_pieces(states, before, after, factors, axis, band_index, band_count):
    members, fields, rows, width = states.shape
    count = lax.axis_size(axis)
    margin = before.shape[2]
    piece = rows // count
    whole = piece % SUBLANES != 0
    extents = (rows,) if whole else (piece,) * count
    place = lax.axis_index(axis).astype(jnp.int32).reshape(1)
    inside = jnp.stack([band_index > 0, band_index < band_count - 1]).astype(jnp.float32)
    found = pl.pallas_call(
        functools.partial(forecast_kernel, count),
        grid=(members,),
        in_specs=[
            pl.BlockSpec(memory_space=pltpu.SMEM),
            pl.BlockSpec(memory_space=pltpu.SMEM),
            pl.BlockSpec(factors.shape, lambda m: (0, 0)),
            pl.BlockSpec((1, fields, rows, width), lambda m: (m, 0, 0, 0)),
            pl.BlockSpec((1, fields, margin, width), lambda m: (m, 0, 0, 0)),
            pl.BlockSpec((1, fields, margin, width), lambda m: (m, 0, 0, 0)),
        ],
        out_specs=[pl.BlockSpec((1, r, width), lambda m: (m, 0, 0)) for r in extents]
        + [pl.BlockSpec((1, fields - 1, r, width), lambda m: (m, 0, 0, 0)) for r in extents],
        out_shape=[jax.ShapeDtypeStruct((members, r, width), jnp.float32) for r in extents]
        + [jax.ShapeDtypeStruct((members, fields - 1, r, width), jnp.float32) for r in extents],
        scratch_shapes=[pltpu.VMEM((fields, factors.shape[0], width), jnp.float32)] * 2,
        cost_estimate=forecast_cost(states, rows),
    )(place, inside, factors, states, before, after)
    if whole:
        return row_pieces(found[0], axis, 1), row_pieces(found[1], axis, 2)
    return list(found[:count]), list(found[count:])


def tapering(cells, grid_width, block_cells, length):
    longitude = cells.astype(jnp.float32)
    tile_total = grid_width // block_cells
    centre = jnp.arange(tile_total).astype(jnp.float32) * block_cells + 0.5 * (block_cells - 1)
    distance = jnp.abs(longitude[..., :, None] - centre)
    distance = jnp.minimum(distance, grid_width - distance)
    return jnp.exp(-0.5 * (distance / length) ** 2)


def member_weights(heights, cells, values, block_cells, length):
    grid_width = heights.shape[-1]
    chosen_cells = (
        cells[:, None, :] == lax.broadcasted_iota(jnp.int32, (1, grid_width, 1), 1)
    ).astype(jnp.float32)
    observed = jnp.einsum("erl,rlo->reo", heights, chosen_cells, precision=lax.Precision.HIGHEST)
    misfit = (values[:, None, :] - observed) ** 2
    taper_weights = tapering(cells, grid_width, block_cells, length)
    likelihood = (
        -0.5
        / OBSERVATION_VARIANCE
        * jnp.einsum("reo,rob->rbe", misfit, taper_weights, precision=lax.Precision.HIGHEST)
    )
    largest = jnp.max(likelihood, axis=-1, keepdims=True)
    scaled = jnp.exp(likelihood - largest)
    return scaled / jnp.sum(scaled, axis=-1, keepdims=True)


def mixing_matrix(weights, draws):
    member_count = weights.shape[-1]
    split = draws.reshape(draws.shape[:-1] + (3, member_count))
    column = lax.broadcasted_iota(jnp.int32, (1, 1, 1, member_count), 3)
    picks = MERGE_FIRST * (split[:, :, 0, :, None] == column).astype(jnp.float32)
    picks = picks + BLEND_COEF_TWO * (split[:, :, 1, :, None] == column).astype(jnp.float32)
    picks = picks + MERGE_THIRD * (split[:, :, 2, :, None] == column).astype(jnp.float32)
    return (1.0 - RELAXATION) * weights[:, :, None, :] + RELAXATION * picks


def merge_fields(members, mixing, block_cells):
    member_count, fields, count_of_rows, grid_width = members.shape
    blocks = members.reshape(
        member_count, fields, count_of_rows, grid_width // block_cells, block_cells
    )
    updated = jnp.einsum("rbek,kfrbc->efrbc", mixing, blocks, precision=lax.Precision.HIGHEST)
    return updated.reshape(member_count, fields, count_of_rows, grid_width)


def by_reach(count):
    return sorted(range(1, count), key=lambda d: abs(2 * d - count))


def send_all(pieces, axis):
    count = lax.axis_size(axis)
    received = [
        lax.ppermute(pieces[d], axis, [(i, (i + d) % count) for i in range(count)])
        for d in range(1, count)
    ]
    own, first = lax.optimization_barrier((pieces[0], received[0]))
    return [own, first] + received[1:]


def row_pieces(array, axis, dim):
    count = lax.axis_size(axis)
    own = lax.axis_index(axis)
    length = array.shape[dim] // count
    return [
        lax.dynamic_slice_in_dim(array, lax.rem(own + d, count) * length, length, axis=dim)
        for d in range(count)
    ]


def put_back(whole, received, axis, field):
    count = lax.axis_size(axis)
    own = lax.axis_index(axis)
    length = received[0].shape[2]
    for d in [0] + by_reach(count)[::-1]:
        piece = received[d]
        start = lax.rem(own + count - d, count) * length
        whole = lax.dynamic_update_slice(whole, piece, (0, field, start, 0))
    return whole


def relative_draws(draws, axis, members_dev):
    count = lax.axis_size(axis)
    own = lax.axis_index(axis)
    distance = lax.rem(own + count - draws // members_dev, count)
    place = distance * members_dev + draws % members_dev
    split = place.reshape(place.shape[:-1] + (3, count, members_dev))
    doubled = jnp.concatenate([split, split], axis=-2)
    turned = lax.dynamic_slice_in_dim(doubled, own, count, axis=-2)
    return turned.reshape(draws.shape)


def body(particle_states, coriolis, observed_cells, observed_values, resample_draws):
    members_dev, _, count_of_rows, _ = particle_states.shape
    count = lax.axis_size("mem")
    band_index = lax.axis_index("dom")
    factors = coriolis_frame(coriolis, band_index, count_of_rows)
    before, after = edge_rows(particle_states, "dom", 2, 2 * STEPS)
    heights, winds = forecast_pieces(
        particle_states, before, after, factors, "mem", band_index, lax.axis_size("dom")
    )
    heights = send_all(heights, "mem")
    winds_all = send_all(winds, "mem")
    heights = jnp.concatenate(heights, axis=0)
    winds_all = jnp.concatenate(winds_all, axis=0)

    cells = observed_cells[0]
    values = observed_values[0]
    draws = relative_draws(resample_draws[0], "mem", members_dev)
    weights = member_weights(heights, cells, values, LBLK, LOC)
    mixing = mixing_matrix(weights, draws)

    def hand_back(members):
        updated = merge_fields(members, mixing, LBLK)
        pieces = [updated[d * members_dev : (d + 1) * members_dev] for d in range(count)]
        return send_all(pieces, "mem")

    analysed = jnp.zeros(particle_states.shape, particle_states.dtype)
    analysed = put_back(analysed, hand_back(heights[:, None]), "mem", 0)
    return put_back(analysed, hand_back(winds_all), "mem", 1)


def solution(mesh):
    return jax.shard_map(
        body,
        mesh=mesh,
        in_specs=(
            P("mem", None, "dom", None),
            P(),
            P("dom", "mem", None),
            P("dom", "mem", None),
            P("dom", "mem", None, None),
        ),
        out_specs=P("mem", None, "dom", None),
        check_vma=False,
    )
```
